256 devices in a mesh: gx: 32 (over x_hi, z, core), gy: 8 (over y, x_lo).
Axes of the slice: x: 4 (x_hi: 2, x_lo: 2; x = x_hi * 2 + x_lo), y: 4, z: 8, core: 2. Of those that a mesh axis runs over, the one named last changes fastest.
Arguments:
- densities: float32 [192, 64, 16, 152], P('gx', 'gy'), may hold values from -6 to 6
- occupancy: int32 [192, 64, 16], P('gx', 'gy'), may hold values from 0 to 4095, as said below
- coarse_local: float32 [96, 32, 8, 152], P('gx', 'gy'), may hold values from -6 to 6
- upward_maps: float32 [8, 152, 152], replicated, may hold values from -0.15625 to 0.15625
- transfer_maps: float32 [16, 152, 152], replicated, may hold values from -0.25 to 0.25
- downward_maps: float32 [8, 152, 152], replicated, may hold values from -0.5 to 0.5
- fine_pairs: int32 [32, 8, 16, 2, 256], P('gx', 'gy'), may hold values from 0 to 2687, as said below
- parent_pairs: int32 [32, 8, 16, 2, 128], P('gx', 'gy'), may hold values from 0 to 719, as said below
Outputs:
- fine_local: float32 [192, 64, 16, 152], P('gx', 'gy')
The draws below stay inside these ranges and needn't reach their ends.
Inputs may be any that keep to these rules, and one draw needn't show every extreme that they name: `occupancy`: A count of 0 marks an empty box. `fine_pairs`: for each device and class, 256 slots: row 0 holds a target among the device's own boxes, row 1 a source in its fine frame, at a translation of that class from the target within the target parent's neighbours' children; both boxes are occupied. Unused slots hold target 6 * 8 * 16 and source 0 and come after the used ones; on some device every slot is used. `parent_pairs`: likewise at the parent level with 128 slots; a parent is occupied where one of its children is. Unused slots hold target (3) * 4 * (8) and source 0 and come after the used ones; on some device every slot is used.
All inputs are finite; a program needn't handle non-finite values.
Results may differ from the reference program's by a relative error of at most 0.0003.
Values sent between devices are 32-bit elements; how exact they have to be, the bound alone decides.
A program may use at most 64 MiB of HBM per device.

```python
import jax
import jax.numpy as jnp
import numpy as np
from jax import lax

COEF = 152
CLASSES = 16
RIM = 3
CX = 6
CY = 8
NZ = 16
CAP_FINE = 256
CAP_PARENT = 128
MESH_X = 32
MESH_Y = 8
NX = 192
NY = 64


def class_table():
    triples = []
    for largest in (2, 3):
        for middle in range(largest + 1):
            for smallest in range(middle + 1):
                triples.append((smallest, middle, largest))
    orderings = ((0, 1, 2), (0, 2, 1), (1, 0, 2), (1, 2, 0), (2, 0, 1), (2, 1, 0))
    table = np.zeros((16, 48, 3), np.int32)
    for number, triple in enumerate(triples):
        signed = set()
        for ordering in orderings:
            for sign_bits in range(8):
                signed.add(tuple(((1 - 2 * (sign_bits >> which & 1)) * triple[ordering[which]] for which in range(3))))
        listed = sorted(signed)
        for column in range(48):
            table[number, column] = listed[column % len(listed)]
    return table


def occupancy_grid(key):
    streams = jax.random.split(jax.random.fold_in(key, 7001), 5)
    hot_x = jax.random.randint(streams[0], (), 1, MESH_X - 1)
    hot_y = jax.random.randint(streams[1], (), 0, MESH_Y)
    levels = jax.random.randint(streams[2], (MESH_X, MESH_Y), 1, 12)
    near_x = jnp.abs(jnp.arange(MESH_X) - hot_x) <= 1
    near_y = jnp.abs(jnp.arange(MESH_Y) - hot_y) <= 1
    levels = jnp.where(near_x[:, None] & near_y[None, :], 16, levels)
    levels = jnp.repeat(jnp.repeat(levels, CX, axis=0), CY, axis=1)
    rolled = jax.random.randint(streams[3], (NX, NY, NZ), 0, 16)
    counts = jax.random.randint(streams[4], (NX, NY, NZ), 1, 4096)
    return jnp.where(rolled < levels[:, :, None], counts, 0)


def choose_spot(key, offsets, lowest, extent, total):
    spots = jnp.arange(extent)
    places = lowest + spots
    goals = places + offsets[..., None]
    fitting = (goals >= 0) & (goals < total)
    thirds = (jnp.abs(offsets) == 3)[..., None]
    parity = jnp.where(offsets[..., None] > 0, places % 2 == 0, places % 2 == 1)
    fitting = fitting & (jnp.logical_not(thirds) | parity)
    noise = jax.random.randint(key, goals.shape, 0, 4096)
    scores = fitting.astype(jnp.int32) * 2 ** 20 + noise * 256 + spots
    chosen = jnp.argmax(scores, axis=-1).astype(jnp.int32)
    return (chosen, jnp.any(fitting, axis=-1))


def level_pairs(key, filled, width_x, width_y, layers, capacity):
    table = jnp.asarray(class_table())
    total_x = width_x * MESH_X
    total_y = width_y * MESH_Y
    frame_y = width_y + 2 * RIM
    unused = width_x * width_y * layers

    def one_device(device):
        place_x = device // MESH_Y
        place_y = device % MESH_Y
        streams = jax.random.split(jax.random.fold_in(key, device), 4)
        picked = jax.random.randint(streams[0], (CLASSES, capacity), 0, 48)
        offsets = table[jnp.arange(CLASSES)[:, None], picked]
        spot_x, good_x = choose_spot(streams[1], offsets[..., 0], place_x * width_x, width_x, total_x)
        spot_y, good_y = choose_spot(streams[2], offsets[..., 1], place_y * width_y, width_y, total_y)
        spot_z, good_z = choose_spot(streams[3], offsets[..., 2], 0, layers, layers)
        global_x = place_x * width_x + spot_x
        global_y = place_y * width_y + spot_y
        source_x = jnp.clip(global_x + offsets[..., 0], 0, total_x - 1)
        source_y = jnp.clip(global_y + offsets[..., 1], 0, total_y - 1)
        source_z = jnp.clip(spot_z + offsets[..., 2], 0, layers - 1)
        live = good_x & good_y & good_z & filled[global_x, global_y, spot_z] & filled[source_x, source_y, source_z]
        targets = jnp.where(live, (spot_x * width_y + spot_y) * layers + spot_z, unused)
        sources = jnp.where(live, ((spot_x + offsets[..., 0] + RIM) * frame_y + spot_y + offsets[..., 1] + RIM) * layers + spot_z + offsets[..., 2], 0)
        ordering = jnp.argsort(jnp.where(live, 0, 1), axis=1, stable=True)
        targets = jnp.take_along_axis(targets, ordering, axis=1)
        sources = jnp.take_along_axis(sources, ordering, axis=1)
        return jnp.stack([targets, sources], axis=1).astype(jnp.int32)
    result = lax.map(one_device, jnp.arange(MESH_X * MESH_Y))
    return result.reshape(MESH_X, MESH_Y, CLASSES, 2, capacity)


def draw_occupancy(key, part):
    return occupancy_grid(key).astype(jnp.int32)


def draw_fine_pairs(key, part):
    filled = occupancy_grid(key) > 0
    return level_pairs(jax.random.fold_in(key, 7002), filled, CX, CY, NZ, CAP_FINE)


def draw_parent_pairs(key, part):
    filled = occupancy_grid(key) > 0
    parent_filled = filled.reshape(NX // 2, 2, NY // 2, 2, NZ // 2, 2).any(axis=(1, 3, 5))
    return level_pairs(jax.random.fold_in(key, 7003), parent_filled, CX // 2, CY // 2, NZ // 2, CAP_PARENT)


def level_of(stream_key, shape, cuts, low, top_value):
    gain, own = 1.0, jax.random.fold_in(stream_key, 6)
    for dim, blocks in cuts:
        heights = jnp.exp(jax.random.uniform(jax.random.fold_in(own, dim), (blocks,), jnp.float32, low / len(cuts), top_value / len(cuts)))
        gain = gain * jnp.repeat(heights, shape[dim] // blocks).reshape([-1 if axis == dim else 1 for axis in range(len(shape))])
    return gain


def centred(rng, shape, scale, most, cuts=(), kind=jnp.bfloat16):
    loudness = level_of(rng, shape, cuts, -0.22, 0.18) if cuts else 1.0
    drawn = jax.random.normal(rng, shape, jnp.float32) * scale * loudness
    return jnp.minimum(jnp.maximum(drawn, -most), most).astype(kind)


def setup_inputs(seed: int = 0) -> dict:
    streams_of = jax.random.split(jax.random.key(seed), 9)
    densities = centred(streams_of[0], (NX, NY, NZ, COEF), 1.0, 6.0, ((0, 32), (1, 8)), jnp.float32)
    occupancy = draw_occupancy(jax.random.fold_in(streams_of[8], 71), 0)
    coarse_local = centred(streams_of[2], (NX // 2, NY // 2, NZ // 2, COEF), 1.0, 6.0, ((0, 32), (1, 8)), jnp.float32)
    upward_maps = centred(streams_of[3], (8, COEF, COEF), (8 * COEF) ** -0.5, 0.15625, (), jnp.float32)
    transfer_maps = centred(streams_of[4], (CLASSES, COEF, COEF), (4 * COEF) ** -0.5, 0.25, (), jnp.float32)
    downward_maps = centred(streams_of[5], (8, COEF, COEF), COEF ** -0.5, 0.5, (), jnp.float32)
    fine_pairs = draw_fine_pairs(jax.random.fold_in(streams_of[8], 71), 0)
    parent_pairs = draw_parent_pairs(jax.random.fold_in(streams_of[8], 71), 0)
    return {"densities": densities, "occupancy": occupancy, "coarse_local": coarse_local, "upward_maps": upward_maps, "transfer_maps": transfer_maps, "downward_maps": downward_maps, "fine_pairs": fine_pairs, "parent_pairs": parent_pairs}


highest = lax.Precision.HIGHEST
level_scale = 0.5


def lift_children(children, upward_maps):
    extent_x, extent_y, extent_z, columns = children.shape
    grouped = children.reshape(extent_x // 2, 2, extent_y // 2, 2, extent_z // 2, 2, columns)
    matrices = upward_maps.reshape(2, 2, 2, columns, columns)
    return jnp.einsum("aibjckp,ijkpq->abcq", grouped, matrices, precision=highest)


def push_down(parents, downward_maps):
    extent_x, extent_y, extent_z, columns = parents.shape
    matrices = downward_maps.reshape(2, 2, 2, columns, columns)
    spread = jnp.einsum("abcp,ijkpq->aibjckq", parents, matrices, precision=highest)
    return spread.reshape(2 * extent_x, 2 * extent_y, 2 * extent_z, columns)


def apply_pairs(framed, pairs, transfer_maps, boxes):
    columns = framed.shape[-1]
    flat_frame = framed.reshape(-1, columns)
    gathered = flat_frame[pairs[:, 1, :]]
    carried = jnp.einsum("csp,cpq->csq", gathered, transfer_maps, precision=highest)
    targets = pairs[:, 0, :].reshape(-1)
    return jnp.zeros((boxes, columns), jnp.float32).at[targets].add(carried.reshape(-1, columns), mode="drop")


def reference(densities, occupancy, coarse_local, upward_maps, transfer_maps, downward_maps, fine_pairs, parent_pairs):
    filled = occupancy > 0
    masked = jnp.where(filled[..., None], densities, jnp.zeros_like(densities))
    reach = 2 * RIM
    padded = jnp.pad(masked, ((reach, reach), (reach, reach), (0, 0), (0, 0)))
    nought = jnp.zeros((), jnp.int32)

    def one_device(device):
        place_x = (device // MESH_Y).astype(jnp.int32)
        place_y = (device % MESH_Y).astype(jnp.int32)
        framed = lax.dynamic_slice(padded, (place_x * CX, place_y * CY, nought, nought), (CX + 2 * reach, CY + 2 * reach, NZ, COEF))
        parent_frame = lift_children(framed, upward_maps)
        fine_frame = framed[RIM:-RIM, RIM:-RIM]
        fine_check = apply_pairs(fine_frame, fine_pairs[place_x, place_y], transfer_maps, CX * CY * NZ)
        own_coarse = lax.dynamic_slice(coarse_local, (place_x * (CX // 2), place_y * (CY // 2), nought, nought), (CX // 2, CY // 2, NZ // 2, COEF))
        parent_boxes = (CX // 2) * (CY // 2) * (NZ // 2)
        parent_local = own_coarse.reshape(-1, COEF) + level_scale * apply_pairs(parent_frame, parent_pairs[place_x, place_y], transfer_maps, parent_boxes)
        fine_local = fine_check.reshape(CX, CY, NZ, COEF) + push_down(parent_local.reshape(CX // 2, CY // 2, NZ // 2, COEF), downward_maps)
        own_filled = lax.dynamic_slice(filled, (place_x * CX, place_y * CY, nought), (CX, CY, NZ))
        return jnp.where(own_filled[..., None], fine_local, jnp.zeros_like(fine_local))

    blocks = lax.map(one_device, jnp.arange(MESH_X * MESH_Y, dtype=jnp.int32))
    blocks = blocks.reshape(MESH_X, MESH_Y, CX, CY, NZ, COEF).transpose(0, 2, 1, 3, 4, 5)
    return blocks.reshape(NX, NY, NZ, COEF)
```

```python
import jax
import jax.numpy as jnp
from jax import lax
from jax.experimental import pallas as pl
from jax.experimental.pallas import tpu as pltpu
from jax.sharding import PartitionSpec as P

f32, bf16, i32 = jnp.float32, jnp.bfloat16, jnp.int32
COEF = 152
CLASSES = 16
CAPF = 256
CAPP = 128
LEVEL_SCALE = 0.5
MESH = pl.DeviceIdType.MESH

TILES = 22


def dot(a, b):
    return lax.dot_general(a, b, (((1,), (0,)), ((), ())), preferred_element_type=f32)


def split(x):
    hi = x.astype(bf16)
    return hi, (x - hi.astype(f32)).astype(bf16)


def stacked(x):
    x = jnp.concatenate([x, jnp.zeros((8, x.shape[1]), f32)], axis=0)
    hi, lo = split(x)
    return jnp.concatenate([hi, lo], axis=0)


def fine_position(s):
    u = s >> 4
    fx = (u * 147) >> 11
    x = fx - 3
    y = u - fx * 14 - 3
    z = s & 15
    below, above = y < 0, y >= 8
    inner = jnp.where(
        below,
        768 + x * 32 + (y + 2) * 16,
        jnp.where(above, 1024 + x * 32 + (y - 8) * 16, x * 128 + y * 16),
    )
    xs = jnp.where(x < 0, x + 2, x - 6)
    base = jnp.where(x < 0, 1280, 1664)
    outer = base + jnp.where(
        below,
        256 + xs * 32 + (y + 2) * 16,
        jnp.where(above, 320 + xs * 32 + (y - 8) * 16, xs * 128 + y * 16),
    )
    return jnp.where((x >= 0) & (x < 6), inner, outer) + z


def parent_position(s):
    u = s >> 3
    fx = (u * 103) >> 10
    x = fx - 3
    y = u - fx * 10 - 3
    z = s & 7
    below, above = y < 0, y >= 4
    base = jnp.where(x < 0, 256, jnp.where(x >= 3, 512, 0))
    xs = jnp.where(x < 0, x + 3, jnp.where(x >= 3, x - 3, x))
    return (
        base
        + jnp.where(
            below,
            128 + xs * 16 + (y + 2) * 8,
            jnp.where(above, 192 + xs * 16 + (y - 4) * 8, xs * 32 + y * 8),
        )
        + z
    )


def kernel(
    shape,
    dens_hbm, occ_ref, coarse_ref, up_hbm, maps_hbm, down_hbm, fp_ref, pp_ref,
    out_ref,
    dens, up, maps, down, occ_pad, rows, frame, frame2, corner, tpad, tmaps, dmaps,
    tgt_pad, tgt_f, tgt_p, pos_f, pos_p, carried_f, carried_p, psum,
    load_sem, send_sem, recv_sem,
):
    mesh_x, mesh_y = shape
    a = lax.axis_index("gx")
    b = lax.axis_index("gy")
    has_l, has_r = a > 0, a < mesh_x - 1
    has_d, has_u = b > 0, b < mesh_y - 1
    left, right = (a - 1, b), (a + 1, b)
    down_n, up_n = (a, b - 1), (a, b + 1)

    loads = [
        pltpu.make_async_copy(src, dst, load_sem.at[n])
        for n, (src, dst) in enumerate(
            [(dens_hbm, dens), (up_hbm, up), (maps_hbm, maps), (down_hbm, down)]
        )
    ]
    for copy in loads:
        copy.start()

    barrier = pltpu.get_barrier_semaphore()
    neighbours = ((has_l, left), (has_r, right), (has_d, down_n), (has_u, up_n))
    for there, who in neighbours:

        @pl.when(there)
        def _():
            pl.semaphore_signal(barrier, inc=1, device_id=who, device_id_type=MESH)

    occ_pad[...] = jnp.zeros_like(occ_pad)
    occ_pad[0:48, 0:16] = (occ_ref[...] > 0).astype(f32)
    mask_t = occ_pad[...].T[0:16, :]
    loads[0].wait()
    rows[1] = jnp.zeros((768, 128), f32)
    for n in range(48):
        keep = mask_t[:, n : n + 1] > 0
        here = dens[n * 16 : n * 16 + 16, :]
        here = jnp.where(keep, here, jnp.zeros_like(here))
        rows[0, n * 16 : n * 16 + 16, :] = here[:, 0:128]
        rows[1, n * 16 : n * 16 + 16, 0 : COEF - 128] = here[:, 128:COEF]

    pl.semaphore_wait(
        barrier, sum(there.astype(i32) for there, _ in neighbours)
    )

    def boxes(at):
        return jnp.concatenate([rows[0, at, :], rows[1, at, :]], axis=1)

    def face(y0, x0, x1):
        return [boxes(pl.ds(x * 128 + y0 * 16, 32)) for x in range(x0, x1)]

    def send(n, src, dst, who):
        return pltpu.make_async_remote_copy(
            src_ref=src, dst_ref=dst, send_sem=send_sem.at[n], recv_sem=recv_sem.at[n],
            device_id=who, device_id_type=MESH,
        )

    ycopies = [
        (send(0, corner.at[0], frame.at[8], down_n), has_d, has_u),
        (send(1, corner.at[2], frame.at[6], up_n), has_u, has_d),
        (send(2, corner.at[1], frame.at[9], down_n), has_d, has_u),
        (send(3, corner.at[3], frame.at[7], up_n), has_u, has_d),
    ]
    xcopies = [
        (send(4, frame.at[pl.ds(0, 2)], frame.at[pl.ds(13, 2)], left), has_l, has_r),
        (send(5, frame.at[pl.ds(4, 2)], frame.at[pl.ds(10, 2)], right), has_r, has_l),
        (send(6, frame.at[16], frame.at[20], left), has_l, has_r),
        (send(7, frame.at[16], frame.at[18], right), has_r, has_l),
    ]
    ccopies = [
        (send(8, corner.at[4], frame.at[15], left), has_l, has_r),
        (send(9, corner.at[5], frame.at[12], right), has_r, has_l),
        (send(10, frame.at[17], frame.at[21], left), has_l, has_r),
        (send(11, frame.at[17], frame.at[19], right), has_r, has_l),
    ]

    def start(copies):
        for copy, sends, _ in copies:

            @pl.when(sends)
            def _():
                copy.start()

    def arrive(copies):
        for copy, _, gets in copies:

            @pl.when(gets)
            def _():
                copy.wait_recv()

    for missing, tiles in (
        (jnp.logical_not(has_d), (6, 7)),
        (jnp.logical_not(has_u), (8, 9)),
        (jnp.logical_not(has_l), (10, 11, 12, 18, 19)),
        (jnp.logical_not(has_r), (13, 14, 15, 20, 21)),
    ):

        @pl.when(missing)
        def _():
            for t in tiles:
                frame[t] = jnp.zeros((COEF, 128), f32)

    def turned(pieces):
        return jnp.concatenate(pieces, axis=0).T[0:COEF, :]

    corner[0] = turned(face(0, 0, 4))
    corner[2] = turned(face(6, 0, 4))
    start(ycopies[0:2])

    loads[1].wait()
    parents = jnp.zeros((96, COEF), f32)
    for k in range(8):
        ci, cj, ck = k >> 2, (k >> 1) & 1, k & 1
        child = jnp.concatenate(
            [
                boxes(pl.ds((2 * px + ci) * 128 + (2 * py + cj) * 16 + ck, 8, stride=2))
                for px in range(3)
                for py in range(4)
            ],
            axis=0,
        )[:, 0:COEF]
        chi, clo = split(child)
        uhi, ulo = split(up[k])
        parents = parents + (dot(chi, uhi) + (dot(clo, uhi) + dot(chi, ulo)))
    pad = jnp.zeros((96, 256 - COEF), f32)
    parents = jnp.concatenate([parents, pad], axis=1)
    for side, y0 in ((0, 0), (1, 2)):
        pieces = face(6 * side, 4, 6)
        pieces += [parents[x * 32 + y0 * 8 : x * 32 + y0 * 8 + 16, :] for x in range(3)]
        pieces += [jnp.zeros((16, 256), f32)]
        corner[2 * side + 1] = turned(pieces)
    start(ycopies[2:4])
    for x in (0, 1, 4, 5):
        frame[x] = boxes(pl.ds(x * 128, 128)).T[0:COEF, :]
    frame[16] = turned([parents, jnp.zeros((32, 256), f32)])
    start(xcopies)
    for x in (2, 3):
        frame[x] = boxes(pl.ds(x * 128, 128)).T[0:COEF, :]

    pos_f[...] = fine_position(fp_ref[:, 1, :])
    pos_p[...] = parent_position(pp_ref[:, 1, :])
    tgt_pad[...] = jnp.zeros_like(tgt_pad)
    tgt_pad[0:16, 0:256] = fp_ref[:, 0, :].astype(f32)
    tgt_pad[0:16, 256:384] = pp_ref[:, 0, :].astype(f32)
    tgt_f[...] = tgt_pad[:, 0:256].T
    tgt_p[...] = tgt_pad[:, 256:384].T
    tpad[...] = jnp.zeros_like(tpad)
    loads[2].wait()

    def turn_map(c, carry):
        m = maps[c]
        hi = m.astype(bf16).astype(f32)
        tpad[0:152, 0:152] = hi
        tpad[160:312, 0:152] = hi
        tpad[320:472, 0:152] = m - hi
        tmaps[c] = tpad[...].T[0:160, :].astype(bf16)
        return carry

    lax.fori_loop(0, CLASSES, turn_map, 0)
    loads[3].wait()
    for k in range(8):
        dhi, dlo = split(down[k])
        dmaps[k, 0] = dhi
        dmaps[k, 1] = dlo
    for t in (0, 1, 2, 3, 4, 5, 16):
        frame2[t] = stacked(frame[t])

    arrive(ycopies)
    lane = lax.broadcasted_iota(i32, (COEF, 128), 1)
    first = lane < 64
    corner[4] = jnp.where(first, frame[6], pltpu.roll(frame[8], 64, 1))
    corner[5] = jnp.where(first, frame[7], pltpu.roll(frame[9], 64, 1))
    frame[17] = jnp.where(first, pltpu.roll(frame[7], 64, 1), frame[9])
    start(ccopies)
    for t in (6, 7, 8, 9, 17):
        frame2[t] = stacked(frame[t])
    arrive(xcopies)
    arrive(ccopies)
    for t in (10, 11, 12, 13, 14, 15, 18, 19, 20, 21):
        frame2[t] = stacked(frame[t])

    sub = lax.broadcasted_iota(i32, (256, 256), 0)

    def pick(first_tile, pairs, place):
        total = None
        for n in range(pairs):
            hot = jnp.where(sub + n * 256 == place, 1.0, 0.0).astype(bf16)
            t = first_tile + 2 * n
            part = dot(jnp.concatenate([frame2[t], frame2[t + 1]], axis=1), hot)
            total = part if total is None else total + part
        return total.astype(bf16)

    def carry_over(c, g):
        g3 = jnp.concatenate(
            [g, g[0:160, :], jnp.zeros((32, g.shape[1]), bf16)], axis=0
        )
        return stacked(dot(tmaps[c], g3)[0:COEF, :])

    def fine_class(c, carry):
        g = pick(0, 8, pos_f[pl.ds(c, 1), :])
        carried_f[c] = carry_over(c, g)
        return carry

    lax.fori_loop(0, CLASSES, fine_class, 0)

    def parent_class(h, carry):
        c = 2 * h
        place = jnp.concatenate([pos_p[pl.ds(c, 1), :], pos_p[pl.ds(c + 1, 1), :]], axis=1)
        g = pick(16, 3, place)
        carried_p[h] = jnp.concatenate(
            [carry_over(c, g[:, 0:128]), carry_over(c + 1, g[:, 128:256])], axis=1
        )
        return carry

    lax.fori_loop(0, CLASSES // 2, parent_class, 0)

    total = None
    plane = lax.broadcasted_iota(i32, (128, 128), 1).astype(f32)
    for h in range(CLASSES // 2):
        hot = jnp.concatenate(
            [
                jnp.where(plane == tgt_p[:, c : c + 1], 1.0, 0.0).astype(bf16)
                for c in (2 * h, 2 * h + 1)
            ],
            axis=0,
        )
        part = dot(carried_p[h], hot)
        total = part if total is None else total + part
    psum[...] = jnp.zeros_like(psum)
    psum[0:COEF, :] = total[0:COEF, :] + total[160:312, :]
    local = coarse_ref[...] + LEVEL_SCALE * psum[...].T[0:96, 0:COEF]
    lhi, llo = split(local)

    fplane = lax.broadcasted_iota(i32, (256, 256), 1).astype(f32)
    for n in range(3):
        total = None
        for c in range(CLASSES):
            hot = jnp.where(fplane + n * 256.0 == tgt_f[:, c : c + 1], 1.0, 0.0).astype(bf16)
            part = dot(carried_f[c], hot)
            total = part if total is None else total + part
        summed = total[0:COEF, :] + total[160:312, :]
        summed = jnp.concatenate([summed, jnp.zeros((104, 256), f32)], axis=0)
        turned_back = summed.T
        rows[0, n * 256 : n * 256 + 256, :] = turned_back[:, 0:128]
        rows[1, n * 256 : n * 256 + 256, :] = turned_back[:, 128:256]

    for k in range(8):
        ci, cj, ck = k >> 2, (k >> 1) & 1, k & 1
        pushed = dot(lhi, dmaps[k, 0]) + (dot(llo, dmaps[k, 0]) + dot(lhi, dmaps[k, 1]))
        pushed = jnp.concatenate([pushed, pad], axis=1)
        for px in range(3):
            for py in range(4):
                at = pl.ds((2 * px + ci) * 128 + (2 * py + cj) * 16 + ck, 8, stride=2)
                n = (px * 4 + py) * 8
                rows[0, at, :] = rows[0, at, :] + pushed[n : n + 8, 0:128]
                rows[1, at, :] = rows[1, at, :] + pushed[n : n + 8, 128:256]
    for n in range(48):
        keep = mask_t[:, n : n + 1] > 0
        here = boxes(pl.ds(n * 16, 16))[:, 0:COEF]
        out_ref[n * 16 : n * 16 + 16, :] = jnp.where(keep, here, jnp.zeros_like(here))

    for copies in (ycopies, xcopies, ccopies):
        for copy, sends, _ in copies:

            @pl.when(sends)
            def _():
                copy.wait_send()


def per_device(shape, dens, occ, coarse, up, maps, down, fp, pp):
    import functools

    anyspace = pl.BlockSpec(memory_space=pl.ANY)
    vmem = pl.BlockSpec(memory_space=pltpu.VMEM)
    out = pl.pallas_call(
        functools.partial(kernel, shape),
        out_shape=jax.ShapeDtypeStruct((768, COEF), f32),
        in_specs=[anyspace, vmem, vmem, anyspace, anyspace, anyspace, vmem, vmem],
        out_specs=vmem,
        scratch_shapes=[
            pltpu.VMEM((768, COEF), f32),
            pltpu.VMEM((8, COEF, COEF), f32),
            pltpu.VMEM((CLASSES, COEF, COEF), f32),
            pltpu.VMEM((8, COEF, COEF), f32),
            pltpu.VMEM((128, 128), f32),
            pltpu.VMEM((2, 768, 128), f32),
            pltpu.VMEM((TILES, COEF, 128), f32),
            pltpu.VMEM((TILES, 320, 128), bf16),
            pltpu.VMEM((6, COEF, 128), f32),
            pltpu.VMEM((512, 256), f32),
            pltpu.VMEM((CLASSES, 160, 512), bf16),
            pltpu.VMEM((8, 2, COEF, COEF), bf16),
            pltpu.VMEM((128, 384), f32),
            pltpu.VMEM((256, 128), f32),
            pltpu.VMEM((128, 128), f32),
            pltpu.VMEM((CLASSES, CAPF), i32),
            pltpu.VMEM((CLASSES, CAPP), i32),
            pltpu.VMEM((CLASSES, 320, CAPF), bf16),
            pltpu.VMEM((CLASSES // 2, 320, 256), bf16),
            pltpu.VMEM((256, 128), f32),
            pltpu.SemaphoreType.DMA((4,)),
            pltpu.SemaphoreType.DMA((12,)),
            pltpu.SemaphoreType.DMA((12,)),
        ],
        compiler_params=pltpu.CompilerParams(
            collective_id=0, has_side_effects=True, vmem_limit_bytes=56 * 1024 * 1024
        ),
    )(
        dens.reshape(768, COEF),
        occ.reshape(48, 16),
        coarse.reshape(96, COEF),
        up,
        maps,
        down,
        fp[0, 0],
        pp[0, 0],
    )
    return out.reshape(dens.shape)


def solution(mesh):
    import functools

    shape = (mesh.shape["gx"], mesh.shape["gy"])
    return jax.shard_map(
        functools.partial(per_device, shape),
        mesh=mesh,
        in_specs=(
            P("gx", "gy", None, None),
            P("gx", "gy", None),
            P("gx", "gy", None, None),
            P(),
            P(),
            P(),
            P("gx", "gy", None, None, None),
            P("gx", "gy", None, None, None),
        ),
        out_specs=P("gx", "gy", None, None),
        check_vma=False,
    )
```

```python
import functools

import jax
import jax.numpy as jnp
from jax import lax
from jax.experimental import pallas as pl
from jax.experimental.pallas import tpu as pltpu
from jax.sharding import PartitionSpec as P

f32, bf16, i32 = jnp.float32, jnp.bfloat16, jnp.int32
COEF = 152
CLASSES = 16
CAPF = 256
CAPP = 128
LEVEL_SCALE = 0.5
MESH = pl.DeviceIdType.MESH

TILES = 22


def dot(a, b):
    return lax.dot_general(a, b, (((1,), (0,)), ((), ())), preferred_element_type=f32)


def split(x):
    hi = x.astype(bf16)
    return hi, (x - hi.astype(f32)).astype(bf16)


def stacked(x):
    hi = x.astype(bf16).astype(f32)
    return jnp.concatenate([hi, x - hi], axis=0).astype(bf16)


def fine_position(s):
    u = s >> 4
    fx = (u * 147) >> 11
    x = fx - 3
    y = u - fx * 14 - 3
    z = s & 15
    below, above = y < 0, y >= 8
    yo = jnp.where(below, y + 2, y - 8) * 16
    middle = (x >= 2) & (x < 4)
    xa = jnp.where(x >= 4, x - 2, x)
    edge = jnp.where(middle, 1536 + (x - 2) * 32, 768 + xa * 32)
    edge = edge + jnp.where(above, 128, 0) + yo
    inner = jnp.where(below | above, edge, x * 128 + y * 16)
    right = x >= 6
    xs = jnp.where(right, x - 6, x + 2)
    side = jnp.where(right, 1280, 1024) + xs * 128 + y * 16
    corner = jnp.where(right, 1920, 1792) + jnp.where(above, 64, 0) + xs * 32 + yo
    outer = jnp.where(below | above, corner, side)
    return jnp.where((x >= 0) & (x < 6), inner, outer) + z


def parent_position(s):
    u = s >> 3
    fx = (u * 103) >> 10
    x = fx - 3
    y = u - fx * 10 - 3
    z = s & 7
    below, above = y < 0, y >= 4
    yo = jnp.where(below, y + 2, y - 4) * 8
    left, right = x < 0, x >= 3
    xs = jnp.where(left, x + 3, jnp.where(right, x - 3, x))
    straight = jnp.where(left, 256, jnp.where(right, 384, 0)) + xs * 32 + y * 8
    corner = jnp.where(left, 512, jnp.where(right, 640, 128)) + jnp.where(above, 64, 0)
    return jnp.where(below | above, corner + xs * 16 + yo, straight) + z


def kernel(
    shape,
    dens_hbm, occ_hbm, coarse_hbm, up_hbm, maps_hbm, down_hbm, fp_hbm, pp_hbm,
    sums, local, dmaps, mask_out,
    dens, up, maps, down, occ, coarse, fp, pp,
    occ_pad, rows, frame, frame2, corner, tpad, tmaps,
    tgt_pad, tgt_f, tgt_p, pos_f, pos_p, picked_f, picked_p, carried_f, carried_p, psum,
    load_sem, send_sem, recv_sem,
):
    mesh_x, mesh_y = shape
    a = lax.axis_index("gx")
    b = lax.axis_index("gy")
    has_l, has_r = a > 0, a < mesh_x - 1
    has_d, has_u = b > 0, b < mesh_y - 1
    left, right = (a - 1, b), (a + 1, b)
    down_n, up_n = (a, b - 1), (a, b + 1)

    barrier = pltpu.get_barrier_semaphore()
    neighbours = ((has_l, left), (has_r, right), (has_d, down_n), (has_u, up_n))
    loads = [
        pltpu.make_async_copy(src, dst, load_sem.at[n])
        for n, (src, dst) in enumerate(
            [
                (occ_hbm, occ), (dens_hbm, dens), (up_hbm, up), (fp_hbm, fp),
                (pp_hbm, pp), (maps_hbm, maps), (down_hbm, down), (coarse_hbm, coarse),
            ]
        )
    ]
    for copy in loads[0:3]:
        copy.start()
    for there, who in neighbours:

        @pl.when(there)
        def _():
            pl.semaphore_signal(barrier, inc=1, device_id=who, device_id_type=MESH)

    for copy in loads[3:]:
        copy.start()

    for missing, tiles in (
        (jnp.logical_not(has_d), (6, 12)),
        (jnp.logical_not(has_u), (7, 13)),
        (jnp.logical_not(has_l), (8, 9, 14, 18, 20)),
        (jnp.logical_not(has_r), (10, 11, 15, 19, 21)),
    ):

        @pl.when(missing)
        def _():
            for t in tiles:
                frame[t] = jnp.zeros((COEF, 128), f32)

    occ_pad[...] = jnp.zeros_like(occ_pad)
    rows[1] = jnp.zeros((768, 128), f32)
    tgt_pad[...] = jnp.zeros_like(tgt_pad)
    tpad[...] = jnp.zeros_like(tpad)
    psum[...] = jnp.zeros_like(psum)

    loads[0].wait()
    occ_pad[0:48, 0:16] = (occ[...] > 0).astype(f32)
    mask_t = occ_pad[...].T[0:16, :]
    mask_out[...] = mask_t
    loads[1].wait()
    for n in range(48):
        keep = mask_t[:, n : n + 1] > 0
        here = dens[n * 16 : n * 16 + 16, :]
        here = jnp.where(keep, here, jnp.zeros_like(here))
        rows[0, n * 16 : n * 16 + 16, :] = here[:, 0:128]
        rows[1, n * 16 : n * 16 + 16, 0 : COEF - 128] = here[:, 128:COEF]

    def boxes(at):
        return jnp.concatenate([rows[0, at, :], rows[1, at, :]], axis=1)

    def face(y0, xs):
        return [boxes(pl.ds(x * 128 + y0 * 16, 32)) for x in xs]

    def send(n, src, dst, who):
        return pltpu.make_async_remote_copy(
            src_ref=src, dst_ref=dst, send_sem=send_sem.at[n], recv_sem=recv_sem.at[n],
            device_id=who, device_id_type=MESH,
        )

    y_first = [
        (send(0, corner.at[0], frame.at[7], down_n), has_d, has_u),
        (send(1, corner.at[1], frame.at[6], up_n), has_u, has_d),
    ]
    y_second = [
        (send(2, corner.at[2], frame.at[13], down_n), has_d, has_u),
        (send(3, corner.at[3], frame.at[12], up_n), has_u, has_d),
    ]
    x_fine = [
        (send(4, frame.at[pl.ds(0, 2)], frame.at[pl.ds(10, 2)], left), has_l, has_r),
        (send(5, frame.at[pl.ds(4, 2)], frame.at[pl.ds(8, 2)], right), has_r, has_l),
    ]
    x_parent = [
        (send(6, frame.at[16], frame.at[19], left), has_l, has_r),
        (send(7, frame.at[16], frame.at[18], right), has_r, has_l),
    ]
    c_fine = [
        (send(8, corner.at[4], frame.at[15], left), has_l, has_r),
        (send(9, corner.at[5], frame.at[14], right), has_r, has_l),
    ]
    c_parent = [
        (send(10, frame.at[17], frame.at[21], left), has_l, has_r),
        (send(11, frame.at[17], frame.at[20], right), has_r, has_l),
    ]

    def start(copies):
        for copy, sends, _ in copies:

            @pl.when(sends)
            def _():
                copy.start()

    def arrive(copies):
        for copy, _, gets in copies:

            @pl.when(gets)
            def _():
                copy.wait_recv()

    def turned(pieces):
        return jnp.concatenate(pieces, axis=0).T[0:COEF, :]

    corner[0] = turned(face(0, (0, 1, 4, 5)))
    corner[1] = turned(face(6, (0, 1, 4, 5)))
    pl.semaphore_wait(barrier, sum(there.astype(i32) for there, _ in neighbours))
    start(y_first)
    for x in (0, 1, 4, 5):
        frame[x] = boxes(pl.ds(x * 128, 128)).T[0:COEF, :]
    start(x_fine)

    loads[2].wait()
    parents = None
    for k in range(8):
        ci, cj, ck = k >> 2, (k >> 1) & 1, k & 1
        child = jnp.concatenate(
            [
                boxes(pl.ds((2 * px + ci) * 128 + (2 * py + cj) * 16 + ck, 8, stride=2))
                for px in range(3)
                for py in range(4)
            ],
            axis=0,
        )[:, 0:COEF]
        chi, clo = split(child)
        uhi, ulo = split(up[k])
        lifted = dot(chi, uhi) + (dot(clo, uhi) + dot(chi, ulo))
        parents = lifted if parents is None else parents + lifted
    parents = jnp.concatenate([parents, jnp.zeros((96, 256 - COEF), f32)], axis=1)
    for side, y0 in ((0, 0), (1, 2)):
        pieces = face(6 * side, (2, 3))
        pieces += [parents[x * 32 + y0 * 8 : x * 32 + y0 * 8 + 16, :] for x in range(3)]
        pieces += [jnp.zeros((16, 256), f32)]
        corner[side + 2] = turned(pieces)
    start(y_second)
    frame[16] = turned([parents, jnp.zeros((32, 256), f32)])
    start(x_parent)
    for x in (2, 3):
        frame[x] = boxes(pl.ds(x * 128, 128)).T[0:COEF, :]

    def doubled(*tiles):
        for t in tiles:
            frame2[t] = stacked(frame[t])

    doubled(0, 1, 2, 3, 4, 5, 16)
    loads[3].wait()
    loads[4].wait()
    pos_f[...] = fine_position(fp[:, 1, :])
    pos_p[...] = parent_position(pp[:, 1, :])
    tgt_pad[0:16, 0:256] = fp[:, 0, :].astype(f32)
    tgt_pad[0:16, 256:384] = pp[:, 0, :].astype(f32)
    tgt_f[...] = tgt_pad[:, 0:256].T
    tgt_p[...] = tgt_pad[:, 256:384].T

    sub = lax.broadcasted_iota(i32, (256, 256), 0)

    def pick(first_tile, pairs, place):
        total = None
        for n in pairs:
            hot = jnp.where(sub == place - n * 256, 1.0, 0.0).astype(bf16)
            t = first_tile + 2 * n
            part = dot(jnp.concatenate([frame2[t], frame2[t + 1]], axis=1), hot)
            total = part if total is None else total + part
        return total.astype(bf16)

    def parent_place(h):
        return jnp.concatenate(
            [pos_p[pl.ds(2 * h, 1), :], pos_p[pl.ds(2 * h + 1, 1), :]], axis=1
        )

    def carry_over(c, g):
        n = g.shape[1]
        g3 = jnp.concatenate([g, g[0:160, :], jnp.zeros((48, n), bf16)], axis=0)
        return stacked(dot(tmaps[c], g3)[0:COEF, :])

    def own_stage(h, carry):
        for c in (2 * h, 2 * h + 1):
            picked_f[c] = pick(0, (0, 1, 2), pos_f[pl.ds(c, 1), :])
        return carry

    lax.fori_loop(0, CLASSES // 2, own_stage, 0)

    arrive(y_first)
    first = lax.broadcasted_iota(i32, (COEF, 128), 1) < 64
    corner[4] = jnp.where(first, frame[6], pltpu.roll(frame[7], 64, 1))
    corner[5] = jnp.where(first, pltpu.roll(frame[6], 64, 1), frame[7])
    start(c_fine)

    loads[5].wait()

    def turn_map(c, carry):
        m = maps[c]
        hi = m.astype(bf16).astype(f32)
        tpad[0:152, 0:152] = hi
        tpad[152:304, 0:152] = hi
        tpad[304:456, 0:152] = m - hi
        tmaps[c] = tpad[...].T[0:160, :].astype(bf16)
        return carry

    lax.fori_loop(0, CLASSES, turn_map, 0)

    arrive(y_second)
    frame[17] = jnp.where(first, pltpu.roll(frame[12], 64, 1), frame[13])
    start(c_parent)

    loads[6].wait()
    for k in range(8):
        dhi, dlo = split(down[k])
        dmaps[k, 0] = dhi
        dmaps[k, 1] = dlo
    arrive(x_fine)
    doubled(6, 7, 8, 9, 10, 11)

    def side_stage(h, carry):
        for c in (2 * h, 2 * h + 1):
            g = pick(0, (3, 4, 5), pos_f[pl.ds(c, 1), :])
            picked_f[c] = picked_f[c] + g
        return carry

    lax.fori_loop(0, CLASSES // 2, side_stage, 0)

    arrive(x_parent)
    arrive(c_fine)
    doubled(12, 13, 14, 15, 17, 18, 19)

    def last_stage(h, carry):
        for c in (2 * h, 2 * h + 1):
            g = picked_f[c] + pick(0, (6, 7), pos_f[pl.ds(c, 1), :])
            carried_f[c] = carry_over(c, g)
        picked_p[h] = pick(16, (0, 1), parent_place(h))
        return carry

    lax.fori_loop(0, CLASSES // 2, last_stage, 0)

    fplane = lax.broadcasted_iota(i32, (256, 256), 1).astype(f32)
    for n in range(3):
        total = None
        for c in range(CLASSES):
            hot = jnp.where(fplane == tgt_f[:, c : c + 1] - n * 256.0, 1.0, 0.0).astype(bf16)
            part = dot(carried_f[c], hot)
            total = part if total is None else total + part
        summed = total[0:COEF, :] + total[COEF : 2 * COEF, :]
        summed = jnp.concatenate([summed, jnp.zeros((104, 256), f32)], axis=0)
        turned_back = summed.T
        sums[0, n * 256 : n * 256 + 256, :] = turned_back[:, 0:128]
        sums[1, n * 256 : n * 256 + 256, :] = turned_back[:, 128:256]

    arrive(c_parent)
    doubled(20, 21)

    def parent_stage(h, carry):
        g = picked_p[h] + pick(16, (2,), parent_place(h))
        carried_p[h] = jnp.concatenate(
            [carry_over(2 * h, g[:, 0:128]), carry_over(2 * h + 1, g[:, 128:256])], axis=1
        )
        return carry

    lax.fori_loop(0, CLASSES // 2, parent_stage, 0, unroll=2)

    total = None
    plane = lax.broadcasted_iota(i32, (128, 128), 1).astype(f32)
    for h in range(CLASSES // 2):
        hot = jnp.concatenate(
            [
                jnp.where(plane == tgt_p[:, c : c + 1], 1.0, 0.0).astype(bf16)
                for c in (2 * h, 2 * h + 1)
            ],
            axis=0,
        )
        part = dot(carried_p[h], hot)
        total = part if total is None else total + part
    psum[0:COEF, :] = total[0:COEF, :] + total[COEF : 2 * COEF, :]
    loads[7].wait()
    expansion = coarse[...] + LEVEL_SCALE * psum[...].T[0:96, 0:COEF]
    lhi, llo = split(expansion)
    local[0] = lhi
    local[1] = llo

    for copies in (y_first, y_second, x_fine, x_parent, c_fine, c_parent):
        for copy, sends, _ in copies:

            @pl.when(sends)
            def _():
                copy.wait_send()


def finish(sums, local, dmaps, mask, out_hbm, rows, out, sem):
    pad = jnp.zeros((96, 256 - COEF), f32)
    lhi, llo = local[0], local[1]
    rows[...] = sums[...]
    pushed = []
    for k in range(8):
        p = dot(lhi, dmaps[k, 0]) + (dot(llo, dmaps[k, 0]) + dot(lhi, dmaps[k, 1]))
        pushed.append(jnp.concatenate([p, pad], axis=1))
    mask_t = mask[...]
    copies = []
    for px in range(3):
        for k in range(8):
            ci, cj, ck = k >> 2, (k >> 1) & 1, k & 1
            for py in range(4):
                at = pl.ds((2 * px + ci) * 128 + (2 * py + cj) * 16 + ck, 8, stride=2)
                n = (px * 4 + py) * 8
                rows[0, at, :] = rows[0, at, :] + pushed[k][n : n + 8, 0:128]
                rows[1, at, :] = rows[1, at, :] + pushed[k][n : n + 8, 128:256]
        for n in range(px * 16, px * 16 + 16):
            keep = mask_t[:, n : n + 1] > 0
            at = pl.ds(n * 16, 16)
            here = jnp.concatenate([rows[0, at, :], rows[1, at, :]], axis=1)[:, 0:COEF]
            out[at, :] = jnp.where(keep, here, jnp.zeros_like(here))
        part = pl.ds(px * 256, 256)
        copy = pltpu.make_async_copy(out.at[part], out_hbm.at[part], sem.at[px])
        copy.start()
        copies.append(copy)
    for copy in copies:
        copy.wait()


def per_device(shape, dens, occ, coarse, up, maps, down, fp, pp):
    vmem = pl.BlockSpec(memory_space=pltpu.VMEM)
    parts = pl.pallas_call(
        functools.partial(kernel, shape),
        out_shape=(
            jax.ShapeDtypeStruct((2, 768, 128), f32),
            jax.ShapeDtypeStruct((2, 96, COEF), bf16),
            jax.ShapeDtypeStruct((8, 2, COEF, COEF), bf16),
            jax.ShapeDtypeStruct((16, 128), f32),
        ),
        in_specs=[pl.BlockSpec(memory_space=pltpu.HBM)] * 8,
        out_specs=(vmem,) * 4,
        scratch_shapes=[
            pltpu.VMEM((768, COEF), f32),
            pltpu.VMEM((8, COEF, COEF), f32),
            pltpu.VMEM((CLASSES, COEF, COEF), f32),
            pltpu.VMEM((8, COEF, COEF), f32),
            pltpu.VMEM((48, 16), i32),
            pltpu.VMEM((96, COEF), f32),
            pltpu.VMEM((CLASSES, 2, CAPF), i32),
            pltpu.VMEM((CLASSES, 2, CAPP), i32),
            pltpu.VMEM((128, 128), f32),
            pltpu.VMEM((2, 768, 128), f32),
            pltpu.VMEM((TILES, COEF, 128), f32),
            pltpu.VMEM((TILES, 2 * COEF, 128), bf16),
            pltpu.VMEM((6, COEF, 128), f32),
            pltpu.VMEM((512, 256), f32),
            pltpu.VMEM((CLASSES, 160, 512), bf16),
            pltpu.VMEM((128, 384), f32),
            pltpu.VMEM((256, 128), f32),
            pltpu.VMEM((128, 128), f32),
            pltpu.VMEM((CLASSES, CAPF), i32),
            pltpu.VMEM((CLASSES, CAPP), i32),
            pltpu.VMEM((CLASSES, 2 * COEF, CAPF), bf16),
            pltpu.VMEM((CLASSES // 2, 2 * COEF, 256), bf16),
            pltpu.VMEM((CLASSES, 2 * COEF, CAPF), bf16),
            pltpu.VMEM((CLASSES // 2, 2 * COEF, 256), bf16),
            pltpu.VMEM((256, 128), f32),
            pltpu.SemaphoreType.DMA((8,)),
            pltpu.SemaphoreType.DMA((12,)),
            pltpu.SemaphoreType.DMA((12,)),
        ],
        compiler_params=pltpu.CompilerParams(
            collective_id=0, has_side_effects=True, vmem_limit_bytes=32 * 1024 * 1024
        ),
    )(
        *[pltpu.with_memory_space_constraint(v, pltpu.HBM) for v in (dens.reshape(768, COEF),
        occ.reshape(48, 16),
        coarse.reshape(96, COEF),
        up,
        maps,
        down,
        fp[0, 0],
        pp[0, 0])],
    )
    out = pl.pallas_call(
        finish,
        out_shape=jax.ShapeDtypeStruct((768, COEF), f32),
        in_specs=[vmem] * 4,
        out_specs=pl.BlockSpec(memory_space=pltpu.HBM),
        scratch_shapes=[
            pltpu.VMEM((2, 768, 128), f32),
            pltpu.VMEM((768, COEF), f32),
            pltpu.SemaphoreType.DMA((3,)),
        ],
        compiler_params=pltpu.CompilerParams(vmem_limit_bytes=8 * 1024 * 1024),
    )(*parts)
    return out.reshape(dens.shape)


def solution(mesh):
    shape = (mesh.shape["gx"], mesh.shape["gy"])
    return jax.shard_map(
        functools.partial(per_device, shape),
        mesh=mesh,
        in_specs=(
            P("gx", "gy", None, None),
            P("gx", "gy", None),
            P("gx", "gy", None, None),
            P(),
            P(),
            P(),
            P("gx", "gy", None, None, None),
            P("gx", "gy", None, None, None),
        ),
        out_specs=P("gx", "gy", None, None),
        check_vma=False,
    )
```

```python
import functools

import jax
import jax.numpy as jnp
from jax import lax
from jax.experimental import pallas as pl
from jax.experimental.pallas import tpu as pltpu
from jax.sharding import PartitionSpec as P

f32, bf16, i32 = jnp.float32, jnp.bfloat16, jnp.int32
COEF = 152
CLASSES = 16
CAPF = 256
CAPP = 128
LEVEL_SCALE = 0.5
MESH = pl.DeviceIdType.MESH

TILES = 22


def dot(a, b):
    return lax.dot_general(a, b, (((1,), (0,)), ((), ())), preferred_element_type=f32)


def split(x):
    hi = x.astype(bf16)
    return hi, (x - hi.astype(f32)).astype(bf16)


def stacked(x):
    hi = x.astype(bf16).astype(f32)
    return jnp.concatenate([hi, x - hi], axis=0).astype(bf16)


def fine_position(s):
    u = s >> 4
    fx = (u * 147) >> 11
    x = fx - 3
    y = u - fx * 14 - 3
    z = s & 15
    below, above = y < 0, y >= 8
    yo = jnp.where(below, y + 2, y - 8) * 16
    middle = (x >= 2) & (x < 4)
    xa = jnp.where(x >= 4, x - 2, x)
    edge = jnp.where(middle, 1536 + (x - 2) * 32, 768 + xa * 32)
    edge = edge + jnp.where(above, 128, 0) + yo
    inner = jnp.where(below | above, edge, x * 128 + y * 16)
    right = x >= 6
    xs = jnp.where(right, x - 6, x + 2)
    side = jnp.where(right, 1280, 1024) + xs * 128 + y * 16
    corner = jnp.where(right, 1920, 1792) + jnp.where(above, 64, 0) + xs * 32 + yo
    outer = jnp.where(below | above, corner, side)
    return jnp.where((x >= 0) & (x < 6), inner, outer) + z


def parent_position(s):
    u = s >> 3
    fx = (u * 103) >> 10
    x = fx - 3
    y = u - fx * 10 - 3
    z = s & 7
    below, above = y < 0, y >= 4
    yo = jnp.where(below, y + 2, y - 4) * 8
    left, right = x < 0, x >= 3
    xs = jnp.where(left, x + 3, jnp.where(right, x - 3, x))
    straight = jnp.where(left, 256, jnp.where(right, 384, 0)) + xs * 32 + y * 8
    corner = jnp.where(left, 512, jnp.where(right, 640, 128)) + jnp.where(above, 64, 0)
    return jnp.where(below | above, corner + xs * 16 + yo, straight) + z


def kernel(
    shape,
    dens_hbm, occ_hbm, coarse_hbm, up_hbm, maps_hbm, down_hbm, fp_hbm, pp_hbm,
    sums, local, dmaps, mask_out,
    dens, up, maps, down, occ, coarse, fp, pp,
    occ_pad, rows, frame, frame2, corner, tpad, tmaps,
    tgt_f, tgt_p, pos_f, pos_p, picked_f, picked_p, carried_f, carried_p, psum,
    load_sem, send_sem, recv_sem,
):
    mesh_x, mesh_y = shape
    a = lax.axis_index("gx")
    b = lax.axis_index("gy")
    has_l, has_r = a > 0, a < mesh_x - 1
    has_d, has_u = b > 0, b < mesh_y - 1
    left, right = (a - 1, b), (a + 1, b)
    down_n, up_n = (a, b - 1), (a, b + 1)

    barrier = pltpu.get_barrier_semaphore()
    neighbours = ((has_l, left), (has_r, right), (has_d, down_n), (has_u, up_n))
    loads = [
        pltpu.make_async_copy(src, dst, load_sem.at[n])
        for n, (src, dst) in enumerate(
            [
                (occ_hbm, occ), (dens_hbm, dens), (up_hbm, up), (fp_hbm, fp),
                (pp_hbm, pp), (maps_hbm, maps), (down_hbm, down), (coarse_hbm, coarse),
            ]
        )
    ]
    for copy in loads[0:3]:
        copy.start()
    for there, who in neighbours:

        @pl.when(there)
        def _():
            pl.semaphore_signal(barrier, inc=1, device_id=who, device_id_type=MESH)

    for copy in loads[3:]:
        copy.start()

    for missing, tiles in (
        (jnp.logical_not(has_d), (6, 12)),
        (jnp.logical_not(has_u), (7, 13)),
        (jnp.logical_not(has_l), (8, 9, 14, 18, 20)),
        (jnp.logical_not(has_r), (10, 11, 15, 19, 21)),
    ):

        @pl.when(missing)
        def _():
            for t in tiles:
                frame[t] = jnp.zeros((COEF, 128), f32)

    occ_pad[...] = jnp.zeros_like(occ_pad)
    rows[1] = jnp.zeros((768, 128), f32)
    tpad[...] = jnp.zeros_like(tpad)
    psum[...] = jnp.zeros_like(psum)

    loads[0].wait()
    occ_pad[0:48, 0:16] = (occ[...] > 0).astype(f32)
    mask_t = occ_pad[...].T[0:16, :]
    mask_out[...] = mask_t
    loads[1].wait()
    for n in range(48):
        keep = mask_t[:, n : n + 1] > 0
        here = dens[n * 16 : n * 16 + 16, :]
        here = jnp.where(keep, here, jnp.zeros_like(here))
        rows[0, n * 16 : n * 16 + 16, :] = here[:, 0:128]
        rows[1, n * 16 : n * 16 + 16, 0 : COEF - 128] = here[:, 128:COEF]

    def boxes(at):
        return jnp.concatenate([rows[0, at, :], rows[1, at, :]], axis=1)

    def face(y0, xs):
        return [boxes(pl.ds(x * 128 + y0 * 16, 32)) for x in xs]

    def send(n, src, dst, who):
        return pltpu.make_async_remote_copy(
            src_ref=src, dst_ref=dst, send_sem=send_sem.at[n], recv_sem=recv_sem.at[n],
            device_id=who, device_id_type=MESH,
        )

    y_first = [
        (send(0, corner.at[0], frame.at[7], down_n), has_d, has_u),
        (send(1, corner.at[1], frame.at[6], up_n), has_u, has_d),
    ]
    y_second = [
        (send(2, corner.at[2], frame.at[13], down_n), has_d, has_u),
        (send(3, corner.at[3], frame.at[12], up_n), has_u, has_d),
    ]
    x_fine = [
        (send(4, frame.at[pl.ds(0, 2)], frame.at[pl.ds(10, 2)], left), has_l, has_r),
        (send(5, frame.at[pl.ds(4, 2)], frame.at[pl.ds(8, 2)], right), has_r, has_l),
    ]
    x_parent = [
        (send(6, frame.at[16], frame.at[19], left), has_l, has_r),
        (send(7, frame.at[16], frame.at[18], right), has_r, has_l),
    ]
    c_fine = [
        (send(8, corner.at[4], frame.at[15], left), has_l, has_r),
        (send(9, corner.at[5], frame.at[14], right), has_r, has_l),
    ]
    c_parent = [
        (send(10, frame.at[17], frame.at[21], left), has_l, has_r),
        (send(11, frame.at[17], frame.at[20], right), has_r, has_l),
    ]

    def start(copies):
        for copy, sends, _ in copies:

            @pl.when(sends)
            def _():
                copy.start()

    def arrive(copies):
        for copy, _, gets in copies:

            @pl.when(gets)
            def _():
                copy.wait_recv()

    def turned(pieces):
        return jnp.concatenate(pieces, axis=0).T[0:COEF, :]

    corner[0] = turned(face(0, (0, 1, 4, 5)))
    corner[1] = turned(face(6, (0, 1, 4, 5)))
    pl.semaphore_wait(barrier, sum(there.astype(i32) for there, _ in neighbours))
    start(y_first)
    for x in (0, 1, 4, 5):
        frame[x] = boxes(pl.ds(x * 128, 128)).T[0:COEF, :]
    start(x_fine)

    loads[2].wait()
    parents = None
    for k in range(8):
        ci, cj, ck = k >> 2, (k >> 1) & 1, k & 1
        child = jnp.concatenate(
            [
                boxes(pl.ds((2 * px + ci) * 128 + (2 * py + cj) * 16 + ck, 8, stride=2))
                for px in range(3)
                for py in range(4)
            ],
            axis=0,
        )[:, 0:COEF]
        chi, clo = split(child)
        uhi, ulo = split(up[k])
        both = dot(jnp.concatenate([chi, clo], axis=0), uhi)
        lifted = both[0:96, :] + (both[96:192, :] + dot(chi, ulo))
        parents = lifted if parents is None else parents + lifted
    parents = jnp.concatenate([parents, jnp.zeros((96, 256 - COEF), f32)], axis=1)
    for side, y0 in ((0, 0), (1, 2)):
        pieces = face(6 * side, (2, 3))
        pieces += [parents[x * 32 + y0 * 8 : x * 32 + y0 * 8 + 16, :] for x in range(3)]
        pieces += [jnp.zeros((16, 256), f32)]
        corner[side + 2] = turned(pieces)
    start(y_second)
    frame[16] = turned([parents, jnp.zeros((32, 256), f32)])
    start(x_parent)
    for x in (2, 3):
        frame[x] = boxes(pl.ds(x * 128, 128)).T[0:COEF, :]

    def doubled(*tiles):
        for t in tiles:
            frame2[t] = stacked(frame[t])

    doubled(0, 1, 2, 3, 4, 5, 16)
    loads[3].wait()
    loads[4].wait()
    pos_f[...] = fine_position(fp[:, 1, :])
    pos_p[...] = parent_position(pp[:, 1, :])

    sub = lax.broadcasted_iota(i32, (256, 256), 0)

    def pick(first_tile, pairs, place):
        total = None
        for n in pairs:
            hot = jnp.where(sub == place - n * 256, 1.0, 0.0).astype(bf16)
            t = first_tile + 2 * n
            part = dot(jnp.concatenate([frame2[t], frame2[t + 1]], axis=1), hot)
            total = part if total is None else total + part
        return total.astype(bf16)

    def parent_place(h):
        return jnp.concatenate(
            [pos_p[pl.ds(2 * h, 1), :], pos_p[pl.ds(2 * h + 1, 1), :]], axis=1
        )

    def carry_over(c, g):
        n = g.shape[1]
        g3 = jnp.concatenate([g, g[0:160, :], jnp.zeros((48, n), bf16)], axis=0)
        return stacked(dot(tmaps[c], g3)[0:COEF, :])

    def turn_map(c, slot):
        m = maps[c]
        hi = m.astype(bf16).astype(f32)
        tpad[slot, 0:152, 0:152] = hi
        tpad[slot, 152:304, 0:152] = hi
        tpad[slot, 304:456, 0:152] = m - hi
        tmaps[c] = tpad[slot].T[0:160, :].astype(bf16)

    loads[5].wait()

    def own_stage(h, carry):
        for n in range(2):
            c = 2 * h + n
            turn_map(c, n)
            picked_f[c] = pick(0, (0, 1, 2), pos_f[pl.ds(c, 1), :])
        return carry

    lax.fori_loop(0, CLASSES // 2, own_stage, 0)

    arrive(y_first)
    first = lax.broadcasted_iota(i32, (COEF, 128), 1) < 64
    corner[4] = jnp.where(first, frame[6], pltpu.roll(frame[7], 64, 1))
    corner[5] = jnp.where(first, pltpu.roll(frame[6], 64, 1), frame[7])
    start(c_fine)

    arrive(y_second)
    frame[17] = jnp.where(first, pltpu.roll(frame[12], 64, 1), frame[13])
    start(c_parent)

    loads[6].wait()
    for k in range(8):
        dhi, dlo = split(down[k])
        dmaps[k, 0] = dhi
        dmaps[k, 1] = dlo
    arrive(x_fine)
    doubled(6, 7, 8, 9, 10, 11)

    def side_stage(h, carry):
        for c in (2 * h, 2 * h + 1):
            g = pick(0, (3, 4, 5), pos_f[pl.ds(c, 1), :])
            picked_f[c] = picked_f[c] + g
            row = fp[pl.ds(c, 1), 0, :].astype(f32)
            tgt_f[c] = jnp.broadcast_to(row, (128, CAPF)).T
            row = pp[pl.ds(c, 1), 0, :].astype(f32)
            tgt_p[c] = jnp.broadcast_to(row, (128, CAPP)).T
        return carry

    lax.fori_loop(0, CLASSES // 2, side_stage, 0)

    arrive(x_parent)
    arrive(c_fine)
    doubled(12, 13, 14, 15, 17, 18, 19)

    def last_stage(h, carry):
        for c in (2 * h, 2 * h + 1):
            picked_f[c] = picked_f[c] + pick(0, (6, 7), pos_f[pl.ds(c, 1), :])
        picked_p[h] = pick(16, (0, 1), parent_place(h))
        return carry

    lax.fori_loop(0, CLASSES // 2, last_stage, 0)

    def transfer_stage(h, carry):
        for n in range(4):
            c = 4 * h + n
            carried_f[c] = carry_over(c, picked_f[c])
        return carry

    lax.fori_loop(0, CLASSES // 4, transfer_stage, 0)

    plane = lax.broadcasted_iota(i32, (256, 128), 1).astype(f32)
    ones, zeros = jnp.ones((256, 128), f32), jnp.zeros((256, 128), f32)
    for n in range(3):
        total = None
        for c in range(CLASSES):
            spread = tgt_f[c]
            hot = jnp.concatenate(
                [
                    jnp.where(plane + (n * 256.0 + m) == spread, ones, zeros).astype(bf16)
                    for m in (0.0, 128.0)
                ],
                axis=1,
            )
            part = dot(carried_f[c], hot)
            total = part if total is None else total + part
        summed = total[0:COEF, :] + total[COEF : 2 * COEF, :]
        summed = jnp.concatenate([summed, jnp.zeros((104, 256), f32)], axis=0)
        turned_back = summed.T
        sums[0, n * 256 : n * 256 + 256, :] = turned_back[:, 0:128]
        sums[1, n * 256 : n * 256 + 256, :] = turned_back[:, 128:256]

    arrive(c_parent)
    doubled(20, 21)

    def parent_stage(q, carry):
        for n in range(4):
            h = 4 * q + n
            picked_p[h] = picked_p[h] + pick(16, (2,), parent_place(h))
        return carry

    lax.fori_loop(0, CLASSES // 8, parent_stage, 0)

    def parent_transfer(q, carry):
        for n in range(2):
            h = 2 * q + n
            g = picked_p[h]
            carried_p[h] = jnp.concatenate(
                [carry_over(2 * h, g[:, 0:128]), carry_over(2 * h + 1, g[:, 128:256])],
                axis=1,
            )
        return carry

    lax.fori_loop(0, CLASSES // 4, parent_transfer, 0)

    total = None
    for h in range(CLASSES // 2):
        hot = jnp.concatenate(
            [
                jnp.where(plane[0:CAPP] == tgt_p[c], 1.0, 0.0).astype(bf16)
                for c in (2 * h, 2 * h + 1)
            ],
            axis=0,
        )
        part = dot(carried_p[h], hot)
        total = part if total is None else total + part
    psum[0:COEF, :] = total[0:COEF, :] + total[COEF : 2 * COEF, :]
    loads[7].wait()
    expansion = coarse[...] + LEVEL_SCALE * psum[...].T[0:96, 0:COEF]
    lhi, llo = split(expansion)
    local[0] = lhi
    local[1] = llo

    for copies in (y_first, y_second, x_fine, x_parent, c_fine, c_parent):
        for copy, sends, _ in copies:

            @pl.when(sends)
            def _():
                copy.wait_send()


def finish(sums, local, dmaps, mask, out_hbm, rows, out, sem):
    pad = jnp.zeros((96, 256 - COEF), f32)
    lhi = local[0]
    lboth = jnp.concatenate([local[0], local[1]], axis=0)
    rows[...] = sums[...]
    pushed = []
    for k in range(8):
        both = dot(lboth, dmaps[k, 0])
        p = both[0:96, :] + (both[96:192, :] + dot(lhi, dmaps[k, 1]))
        pushed.append(jnp.concatenate([p, pad], axis=1))
    mask_t = mask[...]
    copies = []
    for px in range(3):
        for k in range(8):
            ci, cj, ck = k >> 2, (k >> 1) & 1, k & 1
            for py in range(4):
                at = pl.ds((2 * px + ci) * 128 + (2 * py + cj) * 16 + ck, 8, stride=2)
                n = (px * 4 + py) * 8
                rows[0, at, :] = rows[0, at, :] + pushed[k][n : n + 8, 0:128]
                rows[1, at, :] = rows[1, at, :] + pushed[k][n : n + 8, 128:256]
        for n in range(px * 16, px * 16 + 16):
            keep = mask_t[:, n : n + 1] > 0
            at = pl.ds(n * 16, 16)
            here = jnp.concatenate([rows[0, at, :], rows[1, at, :]], axis=1)[:, 0:COEF]
            out[at, :] = jnp.where(keep, here, jnp.zeros_like(here))
        part = pl.ds(px * 256, 256)
        copy = pltpu.make_async_copy(out.at[part], out_hbm.at[part], sem.at[px])
        copy.start()
        copies.append(copy)
    for copy in copies:
        copy.wait()


def per_device(shape, dens, occ, coarse, up, maps, down, fp, pp):
    vmem = pl.BlockSpec(memory_space=pltpu.VMEM)
    parts = pl.pallas_call(
        functools.partial(kernel, shape),
        out_shape=(
            jax.ShapeDtypeStruct((2, 768, 128), f32),
            jax.ShapeDtypeStruct((2, 96, COEF), bf16),
            jax.ShapeDtypeStruct((8, 2, COEF, COEF), bf16),
            jax.ShapeDtypeStruct((16, 128), f32),
        ),
        in_specs=[pl.BlockSpec(memory_space=pltpu.HBM)] * 8,
        out_specs=(vmem,) * 4,
        scratch_shapes=[
            pltpu.VMEM((768, COEF), f32),
            pltpu.VMEM((8, COEF, COEF), f32),
            pltpu.VMEM((CLASSES, COEF, COEF), f32),
            pltpu.VMEM((8, COEF, COEF), f32),
            pltpu.VMEM((48, 16), i32),
            pltpu.VMEM((96, COEF), f32),
            pltpu.VMEM((CLASSES, 2, CAPF), i32),
            pltpu.VMEM((CLASSES, 2, CAPP), i32),
            pltpu.VMEM((128, 128), f32),
            pltpu.VMEM((2, 768, 128), f32),
            pltpu.VMEM((TILES, COEF, 128), f32),
            pltpu.VMEM((TILES, 2 * COEF, 128), bf16),
            pltpu.VMEM((6, COEF, 128), f32),
            pltpu.VMEM((2, 512, 256), f32),
            pltpu.VMEM((CLASSES, 160, 512), bf16),
            pltpu.VMEM((CLASSES, CAPF, 128), f32),
            pltpu.VMEM((CLASSES, CAPP, 128), f32),
            pltpu.VMEM((CLASSES, CAPF), i32),
            pltpu.VMEM((CLASSES, CAPP), i32),
            pltpu.VMEM((CLASSES, 2 * COEF, CAPF), bf16),
            pltpu.VMEM((CLASSES // 2, 2 * COEF, 256), bf16),
            pltpu.VMEM((CLASSES, 2 * COEF, CAPF), bf16),
            pltpu.VMEM((CLASSES // 2, 2 * COEF, 256), bf16),
            pltpu.VMEM((256, 128), f32),
            pltpu.SemaphoreType.DMA((8,)),
            pltpu.SemaphoreType.DMA((12,)),
            pltpu.SemaphoreType.DMA((12,)),
        ],
        compiler_params=pltpu.CompilerParams(
            collective_id=0, has_side_effects=True, vmem_limit_bytes=32 * 1024 * 1024
        ),
    )(
        *[pltpu.with_memory_space_constraint(v, pltpu.HBM) for v in (dens.reshape(768, COEF),
        occ.reshape(48, 16),
        coarse.reshape(96, COEF),
        up,
        maps,
        down,
        fp[0, 0],
        pp[0, 0])],
    )
    out = pl.pallas_call(
        finish,
        out_shape=jax.ShapeDtypeStruct((768, COEF), f32),
        in_specs=[vmem] * 4,
        out_specs=pl.BlockSpec(memory_space=pltpu.HBM),
        scratch_shapes=[
            pltpu.VMEM((2, 768, 128), f32),
            pltpu.VMEM((768, COEF), f32),
            pltpu.SemaphoreType.DMA((3,)),
        ],
        compiler_params=pltpu.CompilerParams(vmem_limit_bytes=8 * 1024 * 1024),
    )(*parts)
    return out.reshape(dens.shape)


def solution(mesh):
    shape = (mesh.shape["gx"], mesh.shape["gy"])
    return jax.shard_map(
        functools.partial(per_device, shape),
        mesh=mesh,
        in_specs=(
            P("gx", "gy", None, None),
            P("gx", "gy", None),
            P("gx", "gy", None, None),
            P(),
            P(),
            P(),
            P("gx", "gy", None, None, None),
            P("gx", "gy", None, None, None),
        ),
        out_specs=P("gx", "gy", None, None),
        check_vma=False,
    )
```

```python
import functools

import jax
import jax.numpy as jnp
from jax import lax
from jax.experimental import pallas as pl
from jax.experimental.pallas import tpu as pltpu
from jax.sharding import PartitionSpec as P

f32, bf16, i32 = jnp.float32, jnp.bfloat16, jnp.int32
COEF = 152
CLASSES = 16
CAPF = 256
CAPP = 128
LEVEL_SCALE = 0.5
MESH = pl.DeviceIdType.MESH

TILES = 22


def dot(a, b):
    return lax.dot_general(a, b, (((1,), (0,)), ((), ())), preferred_element_type=f32)


def split(x):
    hi = x.astype(bf16)
    return hi, (x - hi.astype(f32)).astype(bf16)


def stacked(x):
    hi = x.astype(bf16).astype(f32)
    return jnp.concatenate([hi, x - hi], axis=0).astype(bf16)


def fine_position(s):
    u = s >> 4
    fx = (u * 147) >> 11
    x = fx - 3
    y = u - fx * 14 - 3
    z = s & 15
    below, above = y < 0, y >= 8
    yo = jnp.where(below, y + 2, y - 8) * 16
    middle = (x >= 2) & (x < 4)
    xa = jnp.where(x >= 4, x - 2, x)
    edge = jnp.where(middle, 1536 + (x - 2) * 32, 768 + xa * 32)
    edge = edge + jnp.where(above, 128, 0) + yo
    inner = jnp.where(below | above, edge, x * 128 + y * 16)
    right = x >= 6
    xs = jnp.where(right, x - 6, x + 2)
    side = jnp.where(right, 1280, 1024) + xs * 128 + y * 16
    corner = jnp.where(right, 1920, 1792) + jnp.where(above, 64, 0) + xs * 32 + yo
    outer = jnp.where(below | above, corner, side)
    return jnp.where((x >= 0) & (x < 6), inner, outer) + z


def parent_position(s):
    u = s >> 3
    fx = (u * 103) >> 10
    x = fx - 3
    y = u - fx * 10 - 3
    z = s & 7
    below, above = y < 0, y >= 4
    yo = jnp.where(below, y + 2, y - 4) * 8
    left, right = x < 0, x >= 3
    xs = jnp.where(left, x + 3, jnp.where(right, x - 3, x))
    straight = jnp.where(left, 256, jnp.where(right, 384, 0)) + xs * 32 + y * 8
    corner = jnp.where(left, 512, jnp.where(right, 640, 128)) + jnp.where(above, 64, 0)
    return jnp.where(below | above, corner + xs * 16 + yo, straight) + z


def kernel(
    shape,
    dens_hbm, occ_hbm, coarse_hbm, up_hbm, maps_hbm, down_hbm, fp_hbm, pp_hbm,
    sums, local, dmaps, mask_out,
    dens, up, maps, down, occ, coarse, fp, pp,
    occ_pad, rows, frame, frame2, corner, tpad, tmaps,
    tgt_f, tgt_p, pos_f, pos_p, picked_f, picked_p, carried_f, carried_p, psum,
    load_sem, send_sem, recv_sem,
):
    mesh_x, mesh_y = shape
    a = lax.axis_index("gx")
    b = lax.axis_index("gy")
    has_l, has_r = a > 0, a < mesh_x - 1
    has_d, has_u = b > 0, b < mesh_y - 1
    left, right = (a - 1, b), (a + 1, b)
    down_n, up_n = (a, b - 1), (a, b + 1)

    barrier = pltpu.get_barrier_semaphore()
    neighbours = ((has_l, left), (has_r, right), (has_d, down_n), (has_u, up_n))
    loads = [
        pltpu.make_async_copy(src, dst, load_sem.at[n])
        for n, (src, dst) in enumerate(
            [
                (occ_hbm, occ), (dens_hbm, dens), (up_hbm, up), (fp_hbm, fp),
                (pp_hbm, pp), (maps_hbm, maps), (down_hbm, down), (coarse_hbm, coarse),
            ]
        )
    ]
    for copy in loads[0:3]:
        copy.start()
    for there, who in neighbours:

        @pl.when(there)
        def _():
            pl.semaphore_signal(barrier, inc=1, device_id=who, device_id_type=MESH)

    for copy in loads[3:]:
        copy.start()

    for missing, tiles in (
        (jnp.logical_not(has_d), (6, 12)),
        (jnp.logical_not(has_u), (7, 13)),
        (jnp.logical_not(has_l), (8, 9, 14, 18, 20)),
        (jnp.logical_not(has_r), (10, 11, 15, 19, 21)),
    ):

        @pl.when(missing)
        def _():
            for t in tiles:
                frame[t] = jnp.zeros((COEF, 128), f32)

    occ_pad[...] = jnp.zeros_like(occ_pad)
    rows[1] = jnp.zeros((768, 128), f32)
    tpad[...] = jnp.zeros_like(tpad)
    psum[...] = jnp.zeros_like(psum)

    loads[0].wait()
    occ_pad[0:48, 0:16] = (occ[...] > 0).astype(f32)
    mask_t = occ_pad[...].T[0:16, :]
    mask_out[...] = mask_t
    loads[1].wait()
    for n in range(48):
        keep = mask_t[:, n : n + 1] > 0
        here = dens[n * 16 : n * 16 + 16, :]
        here = jnp.where(keep, here, jnp.zeros_like(here))
        rows[0, n * 16 : n * 16 + 16, :] = here[:, 0:128]
        rows[1, n * 16 : n * 16 + 16, 0 : COEF - 128] = here[:, 128:COEF]

    def boxes(at):
        return jnp.concatenate([rows[0, at, :], rows[1, at, :]], axis=1)

    def face(y0, xs):
        return [boxes(pl.ds(x * 128 + y0 * 16, 32)) for x in xs]

    def send(n, src, dst, who):
        return pltpu.make_async_remote_copy(
            src_ref=src, dst_ref=dst, send_sem=send_sem.at[n], recv_sem=recv_sem.at[n],
            device_id=who, device_id_type=MESH,
        )

    y_first = [
        (send(0, corner.at[0], frame.at[7], down_n), has_d, has_u),
        (send(1, corner.at[1], frame.at[6], up_n), has_u, has_d),
    ]
    y_second = [
        (send(2, corner.at[2], frame.at[13], down_n), has_d, has_u),
        (send(3, corner.at[3], frame.at[12], up_n), has_u, has_d),
    ]
    x_fine = [
        (send(4, frame.at[pl.ds(0, 2)], frame.at[pl.ds(10, 2)], left), has_l, has_r),
        (send(5, frame.at[pl.ds(4, 2)], frame.at[pl.ds(8, 2)], right), has_r, has_l),
    ]
    x_parent = [
        (send(6, frame.at[16], frame.at[19], left), has_l, has_r),
        (send(7, frame.at[16], frame.at[18], right), has_r, has_l),
    ]
    c_fine = [
        (send(8, corner.at[4], frame.at[15], left), has_l, has_r),
        (send(9, corner.at[5], frame.at[14], right), has_r, has_l),
    ]
    c_parent = [
        (send(10, frame.at[17], frame.at[21], left), has_l, has_r),
        (send(11, frame.at[17], frame.at[20], right), has_r, has_l),
    ]

    def start(copies):
        for copy, sends, _ in copies:

            @pl.when(sends)
            def _():
                copy.start()

    def arrive(copies):
        for copy, _, gets in copies:

            @pl.when(gets)
            def _():
                copy.wait_recv()

    def turned(pieces):
        return jnp.concatenate(pieces, axis=0).T[0:COEF, :]

    corner[0] = turned(face(0, (0, 1, 4, 5)))
    corner[1] = turned(face(6, (0, 1, 4, 5)))
    pl.semaphore_wait(barrier, sum(there.astype(i32) for there, _ in neighbours))
    start(y_first)
    for x in (0, 1, 4, 5):
        frame[x] = boxes(pl.ds(x * 128, 128)).T[0:COEF, :]
    start(x_fine)

    loads[2].wait()
    parents = None
    for k in range(8):
        ci, cj, ck = k >> 2, (k >> 1) & 1, k & 1
        child = jnp.concatenate(
            [
                boxes(pl.ds((2 * px + ci) * 128 + (2 * py + cj) * 16 + ck, 8, stride=2))
                for px in range(3)
                for py in range(4)
            ],
            axis=0,
        )[:, 0:COEF]
        chi, clo = split(child)
        uhi, ulo = split(up[k])
        both = dot(jnp.concatenate([chi, clo], axis=0), uhi)
        lifted = both[0:96, :] + (both[96:192, :] + dot(chi, ulo))
        parents = lifted if parents is None else parents + lifted
    parents = jnp.concatenate([parents, jnp.zeros((96, 256 - COEF), f32)], axis=1)
    for side, y0 in ((0, 0), (1, 2)):
        pieces = face(6 * side, (2, 3))
        pieces += [parents[x * 32 + y0 * 8 : x * 32 + y0 * 8 + 16, :] for x in range(3)]
        pieces += [jnp.zeros((16, 256), f32)]
        corner[side + 2] = turned(pieces)
    start(y_second)
    frame[16] = turned([parents, jnp.zeros((32, 256), f32)])
    start(x_parent)
    for x in (2, 3):
        frame[x] = boxes(pl.ds(x * 128, 128)).T[0:COEF, :]

    def doubled(*tiles):
        for t in tiles:
            frame2[t] = stacked(frame[t])

    doubled(0, 1, 2, 3, 4, 5, 16)
    loads[3].wait()
    loads[4].wait()
    pos_f[...] = fine_position(fp[:, 1, :])
    pos_p[...] = parent_position(pp[:, 1, :])

    sub = lax.broadcasted_iota(i32, (256, 256), 0)

    def pick(first_tile, pairs, place):
        total = None
        for n in pairs:
            hot = jnp.where(sub == place - n * 256, 1.0, 0.0).astype(bf16)
            t = first_tile + 2 * n
            part = dot(jnp.concatenate([frame2[t], frame2[t + 1]], axis=1), hot)
            total = part if total is None else total + part
        return total.astype(bf16)

    def parent_place(h):
        return jnp.concatenate(
            [pos_p[pl.ds(2 * h, 1), :], pos_p[pl.ds(2 * h + 1, 1), :]], axis=1
        )

    def carry_over(c, g):
        n = g.shape[1]
        g3 = jnp.concatenate([g, g[0:160, :], jnp.zeros((48, n), bf16)], axis=0)
        return stacked(dot(tmaps[c], g3)[0:COEF, :])

    def turn_map(c, slot):
        m = maps[c]
        hi = m.astype(bf16).astype(f32)
        tpad[slot, 0:152, 0:152] = hi
        tpad[slot, 152:304, 0:152] = hi
        tpad[slot, 304:456, 0:152] = m - hi
        tmaps[c] = tpad[slot].T[0:160, :].astype(bf16)

    loads[5].wait()

    def own_stage(h, carry):
        for n in range(2):
            c = 2 * h + n
            turn_map(c, n)
            picked_f[c] = pick(0, (0, 1, 2), pos_f[pl.ds(c, 1), :])
        return carry

    lax.fori_loop(0, CLASSES // 2, own_stage, 0)

    arrive(y_first)
    first = lax.broadcasted_iota(i32, (COEF, 128), 1) < 64
    corner[4] = jnp.where(first, frame[6], pltpu.roll(frame[7], 64, 1))
    corner[5] = jnp.where(first, pltpu.roll(frame[6], 64, 1), frame[7])
    start(c_fine)

    loads[6].wait()
    for k in range(8):
        dhi, dlo = split(down[k])
        dmaps[k, 0] = dhi
        dmaps[k, 1] = dlo
    arrive(x_fine)
    doubled(6, 7, 8, 9, 10, 11)

    def side_stage(h, carry):
        for c in (2 * h, 2 * h + 1):
            g = pick(0, (3, 4, 5), pos_f[pl.ds(c, 1), :])
            picked_f[c] = picked_f[c] + g
            row = fp[pl.ds(c, 1), 0, :].astype(f32)
            tgt_f[c] = jnp.broadcast_to(row, (128, CAPF)).T
            row = pp[pl.ds(c, 1), 0, :].astype(f32)
            tgt_p[c] = jnp.broadcast_to(row, (128, CAPP)).T
        return carry

    lax.fori_loop(0, CLASSES // 2, side_stage, 0)

    arrive(y_second)
    frame[17] = jnp.where(first, pltpu.roll(frame[12], 64, 1), frame[13])
    start(c_parent)

    arrive(x_parent)
    arrive(c_fine)
    doubled(12, 13, 14, 15, 17, 18, 19)

    def last_stage(h, carry):
        for c in (2 * h, 2 * h + 1):
            picked_f[c] = picked_f[c] + pick(0, (6, 7), pos_f[pl.ds(c, 1), :])
        picked_p[h] = pick(16, (0, 1), parent_place(h))
        return carry

    lax.fori_loop(0, CLASSES // 2, last_stage, 0)

    def transfer_stage(h, carry):
        for n in range(4):
            c = 4 * h + n
            carried_f[c] = carry_over(c, picked_f[c])
        return carry

    lax.fori_loop(0, CLASSES // 4, transfer_stage, 0)

    plane = lax.broadcasted_iota(i32, (256, 128), 1).astype(f32)
    ones, zeros = jnp.ones((256, 128), f32), jnp.zeros((256, 128), f32)
    for n in range(3):
        total = None
        for c in range(CLASSES):
            spread = tgt_f[c]
            hot = jnp.concatenate(
                [
                    jnp.where(plane + (n * 256.0 + m) == spread, ones, zeros).astype(bf16)
                    for m in (0.0, 128.0)
                ],
                axis=1,
            )
            part = dot(carried_f[c], hot)
            total = part if total is None else total + part
        summed = total[0:COEF, :] + total[COEF : 2 * COEF, :]
        summed = jnp.concatenate([summed, jnp.zeros((104, 256), f32)], axis=0)
        turned_back = summed.T
        sums[0, n * 256 : n * 256 + 256, :] = turned_back[:, 0:128]
        sums[1, n * 256 : n * 256 + 256, :] = turned_back[:, 128:256]

    arrive(c_parent)
    doubled(20, 21)

    def parent_stage(q, carry):
        for n in range(4):
            h = 4 * q + n
            picked_p[h] = picked_p[h] + pick(16, (2,), parent_place(h))
        return carry

    lax.fori_loop(0, CLASSES // 8, parent_stage, 0)

    def parent_transfer(q, carry):
        for n in range(2):
            h = 2 * q + n
            g = picked_p[h]
            carried_p[h] = jnp.concatenate(
                [carry_over(2 * h, g[:, 0:128]), carry_over(2 * h + 1, g[:, 128:256])],
                axis=1,
            )
        return carry

    lax.fori_loop(0, CLASSES // 4, parent_transfer, 0)

    total = None
    for h in range(CLASSES // 2):
        hot = jnp.concatenate(
            [
                jnp.where(plane[0:CAPP] == tgt_p[c], 1.0, 0.0).astype(bf16)
                for c in (2 * h, 2 * h + 1)
            ],
            axis=0,
        )
        part = dot(carried_p[h], hot)
        total = part if total is None else total + part
    psum[0:COEF, :] = total[0:COEF, :] + total[COEF : 2 * COEF, :]
    loads[7].wait()
    expansion = coarse[...] + LEVEL_SCALE * psum[...].T[0:96, 0:COEF]
    lhi, llo = split(expansion)
    local[0] = lhi
    local[1] = llo

    for copies in (y_first, y_second, x_fine, x_parent, c_fine, c_parent):
        for copy, sends, _ in copies:

            @pl.when(sends)
            def _():
                copy.wait_send()


def finish(sums, local, dmaps, mask, out_hbm, rows, out, sem):
    pad = jnp.zeros((96, 256 - COEF), f32)
    lhi = local[0]
    lboth = jnp.concatenate([local[0], local[1]], axis=0)
    rows[...] = sums[...]
    pushed = []
    for k in range(8):
        both = dot(lboth, dmaps[k, 0])
        p = both[0:96, :] + (both[96:192, :] + dot(lhi, dmaps[k, 1]))
        pushed.append(jnp.concatenate([p, pad], axis=1))
    mask_t = mask[...]
    copies = []
    for px in range(3):
        for k in range(8):
            ci, cj, ck = k >> 2, (k >> 1) & 1, k & 1
            for py in range(4):
                at = pl.ds((2 * px + ci) * 128 + (2 * py + cj) * 16 + ck, 8, stride=2)
                n = (px * 4 + py) * 8
                rows[0, at, :] = rows[0, at, :] + pushed[k][n : n + 8, 0:128]
                rows[1, at, :] = rows[1, at, :] + pushed[k][n : n + 8, 128:256]
        for n in range(px * 16, px * 16 + 16):
            keep = mask_t[:, n : n + 1] > 0
            at = pl.ds(n * 16, 16)
            here = jnp.concatenate([rows[0, at, :], rows[1, at, :]], axis=1)[:, 0:COEF]
            out[at, :] = jnp.where(keep, here, jnp.zeros_like(here))
        part = pl.ds(px * 256, 256)
        copy = pltpu.make_async_copy(out.at[part], out_hbm.at[part], sem.at[px])
        copy.start()
        copies.append(copy)
    for copy in copies:
        copy.wait()


def per_device(shape, dens, occ, coarse, up, maps, down, fp, pp):
    vmem = pl.BlockSpec(memory_space=pltpu.VMEM)
    parts = pl.pallas_call(
        functools.partial(kernel, shape),
        out_shape=(
            jax.ShapeDtypeStruct((2, 768, 128), f32),
            jax.ShapeDtypeStruct((2, 96, COEF), bf16),
            jax.ShapeDtypeStruct((8, 2, COEF, COEF), bf16),
            jax.ShapeDtypeStruct((16, 128), f32),
        ),
        in_specs=[pl.BlockSpec(memory_space=pltpu.HBM)] * 8,
        out_specs=(vmem,) * 4,
        scratch_shapes=[
            pltpu.VMEM((768, COEF), f32),
            pltpu.VMEM((8, COEF, COEF), f32),
            pltpu.VMEM((CLASSES, COEF, COEF), f32),
            pltpu.VMEM((8, COEF, COEF), f32),
            pltpu.VMEM((48, 16), i32),
            pltpu.VMEM((96, COEF), f32),
            pltpu.VMEM((CLASSES, 2, CAPF), i32),
            pltpu.VMEM((CLASSES, 2, CAPP), i32),
            pltpu.VMEM((128, 128), f32),
            pltpu.VMEM((2, 768, 128), f32),
            pltpu.VMEM((TILES, COEF, 128), f32),
            pltpu.VMEM((TILES, 2 * COEF, 128), bf16),
            pltpu.VMEM((6, COEF, 128), f32),
            pltpu.VMEM((2, 512, 256), f32),
            pltpu.VMEM((CLASSES, 160, 512), bf16),
            pltpu.VMEM((CLASSES, CAPF, 128), f32),
            pltpu.VMEM((CLASSES, CAPP, 128), f32),
            pltpu.VMEM((CLASSES, CAPF), i32),
            pltpu.VMEM((CLASSES, CAPP), i32),
            pltpu.VMEM((CLASSES, 2 * COEF, CAPF), bf16),
            pltpu.VMEM((CLASSES // 2, 2 * COEF, 256), bf16),
            pltpu.VMEM((CLASSES, 2 * COEF, CAPF), bf16),
            pltpu.VMEM((CLASSES // 2, 2 * COEF, 256), bf16),
            pltpu.VMEM((256, 128), f32),
            pltpu.SemaphoreType.DMA((8,)),
            pltpu.SemaphoreType.DMA((12,)),
            pltpu.SemaphoreType.DMA((12,)),
        ],
        compiler_params=pltpu.CompilerParams(
            collective_id=0, has_side_effects=True, vmem_limit_bytes=32 * 1024 * 1024
        ),
    )(
        *[pltpu.with_memory_space_constraint(v, pltpu.HBM) for v in (dens.reshape(768, COEF),
        occ.reshape(48, 16),
        coarse.reshape(96, COEF),
        up,
        maps,
        down,
        fp[0, 0],
        pp[0, 0])],
    )
    out = pl.pallas_call(
        finish,
        out_shape=jax.ShapeDtypeStruct((768, COEF), f32),
        in_specs=[vmem] * 4,
        out_specs=pl.BlockSpec(memory_space=pltpu.HBM),
        scratch_shapes=[
            pltpu.VMEM((2, 768, 128), f32),
            pltpu.VMEM((768, COEF), f32),
            pltpu.SemaphoreType.DMA((3,)),
        ],
        compiler_params=pltpu.CompilerParams(vmem_limit_bytes=8 * 1024 * 1024),
    )(*parts)
    return out.reshape(dens.shape)


def solution(mesh):
    shape = (mesh.shape["gx"], mesh.shape["gy"])
    return jax.shard_map(
        functools.partial(per_device, shape),
        mesh=mesh,
        in_specs=(
            P("gx", "gy", None, None),
            P("gx", "gy", None),
            P("gx", "gy", None, None),
            P(),
            P(),
            P(),
            P("gx", "gy", None, None, None),
            P("gx", "gy", None, None, None),
        ),
        out_specs=P("gx", "gy", None, None),
        check_vma=False,
    )
```

```python
import functools

import jax
import jax.numpy as jnp
from jax import lax
from jax.experimental import pallas as pl
from jax.experimental.pallas import tpu as pltpu
from jax.sharding import PartitionSpec as P

f32, bf16, i32 = jnp.float32, jnp.bfloat16, jnp.int32
COEF = 152
CLASSES = 16
CAPF = 256
CAPP = 128
LEVEL_SCALE = 0.5
MESH = pl.DeviceIdType.MESH

TILES = 22


def dot(a, b):
    return lax.dot_general(a, b, (((1,), (0,)), ((), ())), preferred_element_type=f32)


def split(x):
    hi = x.astype(bf16)
    return hi, (x - hi.astype(f32)).astype(bf16)


def stacked(x):
    hi = x.astype(bf16).astype(f32)
    return jnp.concatenate([hi, x - hi], axis=0).astype(bf16)


def fine_position(s):
    u = s >> 4
    fx = (u * 147) >> 11
    x = fx - 3
    y = u - fx * 14 - 3
    z = s & 15
    below, above = y < 0, y >= 8
    yo = jnp.where(below, y + 2, y - 8) * 16
    middle = (x >= 2) & (x < 4)
    xa = jnp.where(x >= 4, x - 2, x)
    edge = jnp.where(middle, 1536 + (x - 2) * 32, 768 + xa * 32)
    edge = edge + jnp.where(above, 128, 0) + yo
    inner = jnp.where(below | above, edge, x * 128 + y * 16)
    right = x >= 6
    xs = jnp.where(right, x - 6, x + 2)
    side = jnp.where(right, 1280, 1024) + xs * 128 + y * 16
    corner = jnp.where(right, 1920, 1792) + jnp.where(above, 64, 0) + xs * 32 + yo
    outer = jnp.where(below | above, corner, side)
    return jnp.where((x >= 0) & (x < 6), inner, outer) + z


def parent_position(s):
    u = s >> 3
    fx = (u * 103) >> 10
    x = fx - 3
    y = u - fx * 10 - 3
    z = s & 7
    below, above = y < 0, y >= 4
    yo = jnp.where(below, y + 2, y - 4) * 8
    left, right = x < 0, x >= 3
    xs = jnp.where(left, x + 3, jnp.where(right, x - 3, x))
    straight = jnp.where(left, 256, jnp.where(right, 384, 0)) + xs * 32 + y * 8
    corner = jnp.where(left, 512, jnp.where(right, 640, 128)) + jnp.where(above, 64, 0)
    return jnp.where(below | above, corner + xs * 16 + yo, straight) + z


def kernel(
    shape,
    dens_hbm, occ_hbm, coarse_hbm, up_hbm, maps_hbm, down_hbm, fp_hbm, pp_hbm,
    sums, local, dmaps, mask_out,
    dens, up, maps, down, occ, coarse, fp, pp,
    occ_pad, rows, frame, frame2, corner, tpad, tmaps,
    tgt_f, tgt_p, pos_f, pos_p, picked_f, picked_p, carried_f, carried_p, psum,
    load_sem, send_sem, recv_sem,
):
    mesh_x, mesh_y = shape
    a = lax.axis_index("gx")
    b = lax.axis_index("gy")
    has_l, has_r = a > 0, a < mesh_x - 1
    has_d, has_u = b > 0, b < mesh_y - 1
    left, right = (a - 1, b), (a + 1, b)
    down_n, up_n = (a, b - 1), (a, b + 1)

    barrier = pltpu.get_barrier_semaphore()
    neighbours = ((has_l, left), (has_r, right), (has_d, down_n), (has_u, up_n))
    loads = [
        pltpu.make_async_copy(src, dst, load_sem.at[n])
        for n, (src, dst) in enumerate(
            [
                (occ_hbm, occ), (dens_hbm, dens), (up_hbm, up), (fp_hbm, fp),
                (pp_hbm, pp), (maps_hbm, maps), (down_hbm, down), (coarse_hbm, coarse),
            ]
        )
    ]
    for copy in loads[0:3]:
        copy.start()
    for there, who in neighbours:

        @pl.when(there)
        def _():
            pl.semaphore_signal(barrier, inc=1, device_id=who, device_id_type=MESH)

    for copy in loads[3:]:
        copy.start()

    for missing, tiles in (
        (jnp.logical_not(has_d), (6, 12)),
        (jnp.logical_not(has_u), (7, 13)),
        (jnp.logical_not(has_l), (8, 9, 14, 18, 20)),
        (jnp.logical_not(has_r), (10, 11, 15, 19, 21)),
    ):

        @pl.when(missing)
        def _():
            for t in tiles:
                frame[t] = jnp.zeros((COEF, 128), f32)

    occ_pad[...] = jnp.zeros_like(occ_pad)
    rows[1] = jnp.zeros((768, 128), f32)
    tpad[...] = jnp.zeros_like(tpad)
    psum[...] = jnp.zeros_like(psum)

    loads[0].wait()
    occ_pad[0:48, 0:16] = (occ[...] > 0).astype(f32)
    mask_t = occ_pad[...].T[0:16, :]
    mask_out[...] = mask_t
    loads[1].wait()
    for n in range(48):
        keep = mask_t[:, n : n + 1] > 0
        here = dens[n * 16 : n * 16 + 16, :]
        here = jnp.where(keep, here, jnp.zeros_like(here))
        rows[0, n * 16 : n * 16 + 16, :] = here[:, 0:128]
        rows[1, n * 16 : n * 16 + 16, 0 : COEF - 128] = here[:, 128:COEF]

    def boxes(at):
        return jnp.concatenate([rows[0, at, :], rows[1, at, :]], axis=1)

    def face(y0, xs):
        return [boxes(pl.ds(x * 128 + y0 * 16, 32)) for x in xs]

    def send(n, src, dst, who):
        return pltpu.make_async_remote_copy(
            src_ref=src, dst_ref=dst, send_sem=send_sem.at[n], recv_sem=recv_sem.at[n],
            device_id=who, device_id_type=MESH,
        )

    y_first = [
        (send(0, corner.at[0], frame.at[7], down_n), has_d, has_u),
        (send(1, corner.at[1], frame.at[6], up_n), has_u, has_d),
    ]
    y_second = [
        (send(2, corner.at[2], frame.at[13], down_n), has_d, has_u),
        (send(3, corner.at[3], frame.at[12], up_n), has_u, has_d),
    ]
    x_fine = [
        (send(4, frame.at[pl.ds(0, 2)], frame.at[pl.ds(10, 2)], left), has_l, has_r),
        (send(5, frame.at[pl.ds(4, 2)], frame.at[pl.ds(8, 2)], right), has_r, has_l),
    ]
    x_parent = [
        (send(6, frame.at[16], frame.at[19], left), has_l, has_r),
        (send(7, frame.at[16], frame.at[18], right), has_r, has_l),
    ]
    c_fine = [
        (send(8, corner.at[4], frame.at[15], left), has_l, has_r),
        (send(9, corner.at[5], frame.at[14], right), has_r, has_l),
    ]
    c_parent = [
        (send(10, frame.at[17], frame.at[21], left), has_l, has_r),
        (send(11, frame.at[17], frame.at[20], right), has_r, has_l),
    ]

    def start(copies):
        for copy, sends, _ in copies:

            @pl.when(sends)
            def _():
                copy.start()

    def arrive(copies):
        for copy, _, gets in copies:

            @pl.when(gets)
            def _():
                copy.wait_recv()

    def turned(pieces):
        return jnp.concatenate(pieces, axis=0).T[0:COEF, :]

    corner[0] = turned(face(0, (0, 1, 4, 5)))
    corner[1] = turned(face(6, (0, 1, 4, 5)))
    pl.semaphore_wait(barrier, sum(there.astype(i32) for there, _ in neighbours))
    start(y_first)
    for x in (0, 1, 4, 5):
        frame[x] = boxes(pl.ds(x * 128, 128)).T[0:COEF, :]
    start(x_fine)

    loads[2].wait()
    parents = None
    for k in range(8):
        ci, cj, ck = k >> 2, (k >> 1) & 1, k & 1
        child = jnp.concatenate(
            [
                boxes(pl.ds((2 * px + ci) * 128 + (2 * py + cj) * 16 + ck, 8, stride=2))
                for px in range(3)
                for py in range(4)
            ],
            axis=0,
        )[:, 0:COEF]
        chi, clo = split(child)
        uhi, ulo = split(up[k])
        both = dot(jnp.concatenate([chi, clo], axis=0), uhi)
        lifted = both[0:96, :] + (both[96:192, :] + dot(chi, ulo))
        parents = lifted if parents is None else parents + lifted
    parents = jnp.concatenate([parents, jnp.zeros((96, 256 - COEF), f32)], axis=1)
    for side, y0 in ((0, 0), (1, 2)):
        pieces = face(6 * side, (2, 3))
        pieces += [parents[x * 32 + y0 * 8 : x * 32 + y0 * 8 + 16, :] for x in range(3)]
        pieces += [jnp.zeros((16, 256), f32)]
        corner[side + 2] = turned(pieces)
    start(y_second)
    frame[16] = turned([parents, jnp.zeros((32, 256), f32)])
    start(x_parent)
    for x in (2, 3):
        frame[x] = boxes(pl.ds(x * 128, 128)).T[0:COEF, :]

    def doubled(*tiles):
        for t in tiles:
            frame2[t] = stacked(frame[t])

    doubled(0, 1, 2, 3, 4, 5, 16)
    loads[3].wait()
    loads[4].wait()
    pos_f[...] = fine_position(fp[:, 1, :])
    pos_p[...] = parent_position(pp[:, 1, :])

    sub = lax.broadcasted_iota(i32, (256, 256), 0)

    def pick(first_tile, pairs, place):
        total = None
        for n in pairs:
            hot = jnp.where(sub == place - n * 256, 1.0, 0.0).astype(bf16)
            t = first_tile + 2 * n
            part = dot(jnp.concatenate([frame2[t], frame2[t + 1]], axis=1), hot)
            total = part if total is None else total + part
        return total.astype(bf16)

    def parent_place(h):
        return jnp.concatenate(
            [pos_p[pl.ds(2 * h, 1), :], pos_p[pl.ds(2 * h + 1, 1), :]], axis=1
        )

    def by_fours(stage):
        lax.fori_loop(0, CLASSES // 4, lambda q, carry: (stage(q), carry)[1], 0)

    def carry_over(q, n, g):
        g3 = jnp.concatenate(
            [g, g[0:160, :], jnp.zeros((48, g.shape[1]), bf16)], axis=0
        )
        return stacked(dot(tmaps[q, n], g3)[0:COEF, :])

    def turn_map(q, n, slot):
        m = maps[4 * q + n]
        hi = m.astype(bf16).astype(f32)
        tpad[slot, 0:152, 0:152] = hi
        tpad[slot, 152:304, 0:152] = hi
        tpad[slot, 304:456, 0:152] = m - hi
        tmaps[q, n] = tpad[slot].T[0:160, :].astype(bf16)

    loads[5].wait()

    def own_stage(q):
        for n in range(4):
            turn_map(q, n, n % 2)
            picked_f[q, n] = pick(0, (0, 1, 2), pos_f[pl.ds(4 * q + n, 1), :])

    by_fours(own_stage)

    arrive(y_first)
    first = lax.broadcasted_iota(i32, (COEF, 128), 1) < 64
    corner[4] = jnp.where(first, frame[6], pltpu.roll(frame[7], 64, 1))
    corner[5] = jnp.where(first, pltpu.roll(frame[6], 64, 1), frame[7])
    start(c_fine)

    loads[6].wait()
    for k in range(8):
        dhi, dlo = split(down[k])
        dmaps[k, 0] = dhi
        dmaps[k, 1] = dlo
    arrive(x_fine)
    doubled(6, 7, 8, 9, 10, 11)

    def side_stage(q):
        for n in range(4):
            c = 4 * q + n
            g = pick(0, (3, 4, 5), pos_f[pl.ds(c, 1), :])
            picked_f[q, n] = picked_f[q, n] + g
            row = fp[pl.ds(c, 1), 0, :].astype(f32)
            tgt_f[q, n] = jnp.broadcast_to(row, (128, CAPF)).T

    by_fours(side_stage)

    arrive(y_second)
    frame[17] = jnp.where(first, pltpu.roll(frame[12], 64, 1), frame[13])
    start(c_parent)

    arrive(x_parent)
    arrive(c_fine)
    doubled(12, 13, 14, 15, 17, 18, 19)

    def last_stage(q):
        for n in range(4):
            c = 4 * q + n
            picked_f[q, n] = picked_f[q, n] + pick(0, (6, 7), pos_f[pl.ds(c, 1), :])
            row = pp[pl.ds(c, 1), 0, :].astype(f32)
            tgt_p[q, n] = jnp.broadcast_to(row, (128, CAPP)).T
        for m in range(2):
            picked_p[q, m] = pick(16, (0, 1), parent_place(2 * q + m))

    by_fours(last_stage)

    def transfer_stage(q):
        for n in range(4):
            carried_f[q, n] = carry_over(q, n, picked_f[q, n])

    by_fours(transfer_stage)

    plane = lax.broadcasted_iota(i32, (256, 128), 1).astype(f32)
    ones, zeros = jnp.ones((256, 128), f32), jnp.zeros((256, 128), f32)
    for n in range(3):
        total = None
        for c in range(CLASSES):
            spread = tgt_f[c // 4, c % 4]
            hot = jnp.concatenate(
                [
                    jnp.where(plane + (n * 256.0 + m) == spread, ones, zeros).astype(bf16)
                    for m in (0.0, 128.0)
                ],
                axis=1,
            )
            part = dot(carried_f[c // 4, c % 4], hot)
            total = part if total is None else total + part
        summed = total[0:COEF, :] + total[COEF : 2 * COEF, :]
        summed = jnp.concatenate([summed, jnp.zeros((104, 256), f32)], axis=0)
        turned_back = summed.T
        sums[0, n * 256 : n * 256 + 256, :] = turned_back[:, 0:128]
        sums[1, n * 256 : n * 256 + 256, :] = turned_back[:, 128:256]

    arrive(c_parent)
    doubled(20, 21)

    def parent_stage(q):
        for m in range(2):
            g = pick(16, (2,), parent_place(2 * q + m))
            picked_p[q, m] = picked_p[q, m] + g

    by_fours(parent_stage)

    def parent_transfer(q):
        for m in range(2):
            g = picked_p[q, m]
            carried_p[q, m] = jnp.concatenate(
                [carry_over(q, 2 * m, g[:, 0:128]), carry_over(q, 2 * m + 1, g[:, 128:256])],
                axis=1,
            )

    by_fours(parent_transfer)

    total = None
    for h in range(CLASSES // 2):
        hot = jnp.concatenate(
            [
                jnp.where(plane[0:CAPP] == tgt_p[c // 4, c % 4], 1.0, 0.0).astype(bf16)
                for c in (2 * h, 2 * h + 1)
            ],
            axis=0,
        )
        part = dot(carried_p[h // 2, h % 2], hot)
        total = part if total is None else total + part
    psum[0:COEF, :] = total[0:COEF, :] + total[COEF : 2 * COEF, :]
    loads[7].wait()
    expansion = coarse[...] + LEVEL_SCALE * psum[...].T[0:96, 0:COEF]
    lhi, llo = split(expansion)
    local[0] = lhi
    local[1] = llo

    for copies in (y_first, y_second, x_fine, x_parent, c_fine, c_parent):
        for copy, sends, _ in copies:

            @pl.when(sends)
            def _():
                copy.wait_send()


def finish(sums, local, dmaps, mask, out_hbm, rows, out, sem):
    pad = jnp.zeros((96, 256 - COEF), f32)
    lhi = local[0]
    lboth = jnp.concatenate([local[0], local[1]], axis=0)
    rows[...] = sums[...]
    pushed = []
    for k in range(8):
        both = dot(lboth, dmaps[k, 0])
        p = both[0:96, :] + (both[96:192, :] + dot(lhi, dmaps[k, 1]))
        pushed.append(jnp.concatenate([p, pad], axis=1))
    mask_t = mask[...]
    copies = []
    for px in range(3):
        for k in range(8):
            ci, cj, ck = k >> 2, (k >> 1) & 1, k & 1
            for py in range(4):
                at = pl.ds((2 * px + ci) * 128 + (2 * py + cj) * 16 + ck, 8, stride=2)
                n = (px * 4 + py) * 8
                rows[0, at, :] = rows[0, at, :] + pushed[k][n : n + 8, 0:128]
                rows[1, at, :] = rows[1, at, :] + pushed[k][n : n + 8, 128:256]
        for n in range(px * 16, px * 16 + 16):
            keep = mask_t[:, n : n + 1] > 0
            at = pl.ds(n * 16, 16)
            here = jnp.concatenate([rows[0, at, :], rows[1, at, :]], axis=1)[:, 0:COEF]
            out[at, :] = jnp.where(keep, here, jnp.zeros_like(here))
        part = pl.ds(px * 256, 256)
        copy = pltpu.make_async_copy(out.at[part], out_hbm.at[part], sem.at[px])
        copy.start()
        copies.append(copy)
    for copy in copies:
        copy.wait()


def per_device(shape, dens, occ, coarse, up, maps, down, fp, pp):
    vmem = pl.BlockSpec(memory_space=pltpu.VMEM)
    parts = pl.pallas_call(
        functools.partial(kernel, shape),
        out_shape=(
            jax.ShapeDtypeStruct((2, 768, 128), f32),
            jax.ShapeDtypeStruct((2, 96, COEF), bf16),
            jax.ShapeDtypeStruct((8, 2, COEF, COEF), bf16),
            jax.ShapeDtypeStruct((16, 128), f32),
        ),
        in_specs=[pl.BlockSpec(memory_space=pltpu.HBM)] * 8,
        out_specs=(vmem,) * 4,
        scratch_shapes=[
            pltpu.VMEM((768, COEF), f32),
            pltpu.VMEM((8, COEF, COEF), f32),
            pltpu.VMEM((CLASSES, COEF, COEF), f32),
            pltpu.VMEM((8, COEF, COEF), f32),
            pltpu.VMEM((48, 16), i32),
            pltpu.VMEM((96, COEF), f32),
            pltpu.VMEM((CLASSES, 2, CAPF), i32),
            pltpu.VMEM((CLASSES, 2, CAPP), i32),
            pltpu.VMEM((128, 128), f32),
            pltpu.VMEM((2, 768, 128), f32),
            pltpu.VMEM((TILES, COEF, 128), f32),
            pltpu.VMEM((TILES, 2 * COEF, 128), bf16),
            pltpu.VMEM((6, COEF, 128), f32),
            pltpu.VMEM((2, 512, 256), f32),
            pltpu.VMEM((4, 4, 160, 512), bf16),
            pltpu.VMEM((4, 4, CAPF, 128), f32),
            pltpu.VMEM((4, 4, CAPP, 128), f32),
            pltpu.VMEM((CLASSES, CAPF), i32),
            pltpu.VMEM((CLASSES, CAPP), i32),
            pltpu.VMEM((4, 4, 2 * COEF, CAPF), bf16),
            pltpu.VMEM((4, 2, 2 * COEF, 256), bf16),
            pltpu.VMEM((4, 4, 2 * COEF, CAPF), bf16),
            pltpu.VMEM((4, 2, 2 * COEF, 256), bf16),
            pltpu.VMEM((256, 128), f32),
            pltpu.SemaphoreType.DMA((8,)),
            pltpu.SemaphoreType.DMA((12,)),
            pltpu.SemaphoreType.DMA((12,)),
        ],
        compiler_params=pltpu.CompilerParams(
            collective_id=0, has_side_effects=True, vmem_limit_bytes=32 * 1024 * 1024
        ),
    )(
        *[pltpu.with_memory_space_constraint(v, pltpu.HBM) for v in (dens.reshape(768, COEF),
        occ.reshape(48, 16),
        coarse.reshape(96, COEF),
        up,
        maps,
        down,
        fp[0, 0],
        pp[0, 0])],
    )
    out = pl.pallas_call(
        finish,
        out_shape=jax.ShapeDtypeStruct((768, COEF), f32),
        in_specs=[vmem] * 4,
        out_specs=pl.BlockSpec(memory_space=pltpu.HBM),
        scratch_shapes=[
            pltpu.VMEM((2, 768, 128), f32),
            pltpu.VMEM((768, COEF), f32),
            pltpu.SemaphoreType.DMA((3,)),
        ],
        compiler_params=pltpu.CompilerParams(vmem_limit_bytes=8 * 1024 * 1024),
    )(*parts)
    return out.reshape(dens.shape)


def solution(mesh):
    shape = (mesh.shape["gx"], mesh.shape["gy"])
    return jax.shard_map(
        functools.partial(per_device, shape),
        mesh=mesh,
        in_specs=(
            P("gx", "gy", None, None),
            P("gx", "gy", None),
            P("gx", "gy", None, None),
            P(),
            P(),
            P(),
            P("gx", "gy", None, None, None),
            P("gx", "gy", None, None, None),
        ),
        out_specs=P("gx", "gy", None, None),
        check_vma=False,
    )
```

```python
import functools

import jax
import jax.numpy as jnp
from jax import lax
from jax.experimental import pallas as pl
from jax.experimental.pallas import tpu as pltpu
from jax.sharding import PartitionSpec as P

f32, bf16, i32 = jnp.float32, jnp.bfloat16, jnp.int32
COEF = 152
CLASSES = 16
CAPF = 256
CAPP = 128
LEVEL_SCALE = 0.5
MESH = pl.DeviceIdType.MESH

TILES = 22


def dot(a, b):
    return lax.dot_general(a, b, (((1,), (0,)), ((), ())), preferred_element_type=f32)


def split(x):
    hi = x.astype(bf16)
    return hi, (x - hi.astype(f32)).astype(bf16)


def stacked(x):
    hi = x.astype(bf16).astype(f32)
    return jnp.concatenate([hi, x - hi], axis=0).astype(bf16)


def fine_position(s):
    u = s >> 4
    fx = (u * 147) >> 11
    x = fx - 3
    y = u - fx * 14 - 3
    z = s & 15
    below, above = y < 0, y >= 8
    yo = jnp.where(below, y + 2, y - 8) * 16
    middle = (x >= 2) & (x < 4)
    xa = jnp.where(x >= 4, x - 2, x)
    edge = jnp.where(middle, 1536 + (x - 2) * 32, 768 + xa * 32)
    edge = edge + jnp.where(above, 128, 0) + yo
    inner = jnp.where(below | above, edge, x * 128 + y * 16)
    right = x >= 6
    xs = jnp.where(right, x - 6, x + 2)
    side = jnp.where(right, 1280, 1024) + xs * 128 + y * 16
    corner = jnp.where(right, 1920, 1792) + jnp.where(above, 64, 0) + xs * 32 + yo
    outer = jnp.where(below | above, corner, side)
    return jnp.where((x >= 0) & (x < 6), inner, outer) + z


def parent_position(s):
    u = s >> 3
    fx = (u * 103) >> 10
    x = fx - 3
    y = u - fx * 10 - 3
    z = s & 7
    below, above = y < 0, y >= 4
    yo = jnp.where(below, y + 2, y - 4) * 8
    left, right = x < 0, x >= 3
    xs = jnp.where(left, x + 3, jnp.where(right, x - 3, x))
    straight = jnp.where(left, 256, jnp.where(right, 384, 0)) + xs * 32 + y * 8
    corner = jnp.where(left, 512, jnp.where(right, 640, 128)) + jnp.where(above, 64, 0)
    return jnp.where(below | above, corner + xs * 16 + yo, straight) + z


def kernel(
    shape,
    dens_hbm, occ_hbm, coarse_hbm, up_hbm, maps_hbm, down_hbm, fp_hbm, pp_hbm,
    sums, local, dmaps, mask_out,
    dens, up, maps, down, occ, coarse, fp, pp,
    occ_pad, rows, frame, frame2, corner, tpad, tmaps,
    tgt_f, tgt_p, pos_f, pos_p, picked_f, picked_p, carried_f, carried_p, psum,
    load_sem, send_sem, recv_sem,
):
    mesh_x, mesh_y = shape
    a = lax.axis_index("gx")
    b = lax.axis_index("gy")
    has_l, has_r = a > 0, a < mesh_x - 1
    has_d, has_u = b > 0, b < mesh_y - 1
    left, right = (a - 1, b), (a + 1, b)
    down_n, up_n = (a, b - 1), (a, b + 1)

    barrier = pltpu.get_barrier_semaphore()
    neighbours = ((has_l, left), (has_r, right), (has_d, down_n), (has_u, up_n))
    loads = [
        pltpu.make_async_copy(src, dst, load_sem.at[n])
        for n, (src, dst) in enumerate(
            [
                (occ_hbm, occ), (dens_hbm, dens), (up_hbm, up), (fp_hbm, fp),
                (pp_hbm, pp), (maps_hbm, maps), (down_hbm, down), (coarse_hbm, coarse),
            ]
        )
    ]
    for copy in loads[0:3]:
        copy.start()
    for there, who in neighbours:

        @pl.when(there)
        def _():
            pl.semaphore_signal(barrier, inc=1, device_id=who, device_id_type=MESH)

    for copy in loads[3:]:
        copy.start()

    for missing, tiles in (
        (jnp.logical_not(has_d), (6, 12)),
        (jnp.logical_not(has_u), (7, 13)),
        (jnp.logical_not(has_l), (8, 9, 14, 18, 20)),
        (jnp.logical_not(has_r), (10, 11, 15, 19, 21)),
    ):

        @pl.when(missing)
        def _():
            for t in tiles:
                frame[t] = jnp.zeros((COEF, 128), f32)

    occ_pad[...] = jnp.zeros_like(occ_pad)
    rows[1] = jnp.zeros((768, 128), f32)
    tpad[...] = jnp.zeros_like(tpad)
    psum[...] = jnp.zeros_like(psum)

    loads[0].wait()
    occ_pad[0:48, 0:16] = (occ[...] > 0).astype(f32)
    mask_t = occ_pad[...].T[0:16, :]
    mask_out[...] = mask_t
    loads[1].wait()
    for n in range(48):
        keep = mask_t[:, n : n + 1] > 0
        here = dens[n * 16 : n * 16 + 16, :]
        here = jnp.where(keep, here, jnp.zeros_like(here))
        rows[0, n * 16 : n * 16 + 16, :] = here[:, 0:128]
        rows[1, n * 16 : n * 16 + 16, 0 : COEF - 128] = here[:, 128:COEF]

    def boxes(at):
        return jnp.concatenate([rows[0, at, :], rows[1, at, :]], axis=1)

    def face(y0, xs):
        return [boxes(pl.ds(x * 128 + y0 * 16, 32)) for x in xs]

    def send(n, src, dst, who):
        return pltpu.make_async_remote_copy(
            src_ref=src, dst_ref=dst, send_sem=send_sem.at[n], recv_sem=recv_sem.at[n],
            device_id=who, device_id_type=MESH,
        )

    y_first = [
        (send(0, corner.at[0], frame.at[7], down_n), has_d, has_u),
        (send(1, corner.at[1], frame.at[6], up_n), has_u, has_d),
    ]
    y_second = [
        (send(2, corner.at[2], frame.at[13], down_n), has_d, has_u),
        (send(3, corner.at[3], frame.at[12], up_n), has_u, has_d),
    ]
    x_fine = [
        (send(4, frame.at[pl.ds(0, 2)], frame.at[pl.ds(10, 2)], left), has_l, has_r),
        (send(5, frame.at[pl.ds(4, 2)], frame.at[pl.ds(8, 2)], right), has_r, has_l),
    ]
    x_parent = [
        (send(6, frame.at[16], frame.at[19], left), has_l, has_r),
        (send(7, frame.at[16], frame.at[18], right), has_r, has_l),
    ]
    c_fine = [
        (send(8, corner.at[4], frame.at[15], left), has_l, has_r),
        (send(9, corner.at[5], frame.at[14], right), has_r, has_l),
    ]
    c_parent = [
        (send(10, frame.at[17], frame.at[21], left), has_l, has_r),
        (send(11, frame.at[17], frame.at[20], right), has_r, has_l),
    ]

    def start(copies):
        for copy, sends, _ in copies:

            @pl.when(sends)
            def _():
                copy.start()

    def arrive(copies):
        for copy, _, gets in copies:

            @pl.when(gets)
            def _():
                copy.wait_recv()

    def turned(pieces):
        return jnp.concatenate(pieces, axis=0).T[0:COEF, :]

    corner[0] = turned(face(0, (0, 1, 4, 5)))
    corner[1] = turned(face(6, (0, 1, 4, 5)))
    pl.semaphore_wait(barrier, sum(there.astype(i32) for there, _ in neighbours))
    start(y_first)
    for x in (0, 1, 4, 5):
        frame[x] = boxes(pl.ds(x * 128, 128)).T[0:COEF, :]
    start(x_fine)

    loads[2].wait()
    parents = None
    for k in range(8):
        ci, cj, ck = k >> 2, (k >> 1) & 1, k & 1
        child = jnp.concatenate(
            [
                boxes(pl.ds((2 * px + ci) * 128 + (2 * py + cj) * 16 + ck, 8, stride=2))
                for px in range(3)
                for py in range(4)
            ],
            axis=0,
        )[:, 0:COEF]
        chi, clo = split(child)
        uhi, ulo = split(up[k])
        both = dot(jnp.concatenate([chi, clo], axis=0), uhi)
        lifted = both[0:96, :] + (both[96:192, :] + dot(chi, ulo))
        parents = lifted if parents is None else parents + lifted
    parents = jnp.concatenate([parents, jnp.zeros((96, 256 - COEF), f32)], axis=1)
    for side, y0 in ((0, 0), (1, 2)):
        pieces = face(6 * side, (2, 3))
        pieces += [parents[x * 32 + y0 * 8 : x * 32 + y0 * 8 + 16, :] for x in range(3)]
        pieces += [jnp.zeros((16, 256), f32)]
        corner[side + 2] = turned(pieces)
    start(y_second)
    frame[16] = turned([parents, jnp.zeros((32, 256), f32)])
    start(x_parent)
    for x in (2, 3):
        frame[x] = boxes(pl.ds(x * 128, 128)).T[0:COEF, :]

    def doubled(*tiles):
        for t in tiles:
            frame2[t] = stacked(frame[t])

    doubled(0, 1, 2, 3, 4, 5, 16)
    loads[3].wait()
    loads[4].wait()
    pos_f[...] = fine_position(fp[:, 1, :])
    pos_p[...] = parent_position(pp[:, 1, :])

    sub = lax.broadcasted_iota(i32, (256, 256), 0)

    def pick(first_tile, pairs, place):
        total = None
        for n in pairs:
            hot = jnp.where(sub == place - n * 256, 1.0, 0.0).astype(bf16)
            t = first_tile + 2 * n
            part = dot(jnp.concatenate([frame2[t], frame2[t + 1]], axis=1), hot)
            total = part if total is None else total + part
        return total.astype(bf16)

    def parent_place(h):
        return jnp.concatenate(
            [pos_p[pl.ds(2 * h, 1), :], pos_p[pl.ds(2 * h + 1, 1), :]], axis=1
        )

    def by_fours(stage, unroll=1):
        lax.fori_loop(
            0, CLASSES // 4, lambda q, carry: (stage(q), carry)[1], 0, unroll=unroll
        )

    def carry_over(q, n, g):
        g3 = jnp.concatenate(
            [g, g[0:160, :], jnp.zeros((48, g.shape[1]), bf16)], axis=0
        )
        return stacked(dot(tmaps[q, n], g3)[0:COEF, :])

    def turn_map(q, n, slot):
        m = maps[4 * q + n]
        hi = m.astype(bf16).astype(f32)
        tpad[slot, 0:152, 0:152] = hi
        tpad[slot, 152:304, 0:152] = hi
        tpad[slot, 304:456, 0:152] = m - hi
        tmaps[q, n] = tpad[slot].T[0:160, :].astype(bf16)

    loads[5].wait()

    def own_stage(q):
        for n in range(4):
            turn_map(q, n, n % 2)
            picked_f[q, n] = pick(0, (0, 1, 2), pos_f[pl.ds(4 * q + n, 1), :])

    by_fours(own_stage)

    arrive(y_first)
    first = lax.broadcasted_iota(i32, (COEF, 128), 1) < 64
    corner[4] = jnp.where(first, frame[6], pltpu.roll(frame[7], 64, 1))
    corner[5] = jnp.where(first, pltpu.roll(frame[6], 64, 1), frame[7])
    start(c_fine)

    loads[6].wait()
    for k in range(8):
        dhi, dlo = split(down[k])
        dmaps[k, 0] = dhi
        dmaps[k, 1] = dlo
    arrive(x_fine)
    doubled(6, 7, 8, 9, 10, 11)

    def side_stage(q):
        for n in range(4):
            c = 4 * q + n
            g = pick(0, (3, 4, 5), pos_f[pl.ds(c, 1), :])
            picked_f[q, n] = picked_f[q, n] + g
            row = fp[pl.ds(c, 1), 0, :].astype(f32)
            tgt_f[q, n] = jnp.broadcast_to(row, (128, CAPF)).T

    by_fours(side_stage)

    arrive(y_second)
    frame[17] = jnp.where(first, pltpu.roll(frame[12], 64, 1), frame[13])
    start(c_parent)

    arrive(x_parent)
    arrive(c_fine)
    doubled(12, 13, 14, 15, 17, 18, 19)

    def last_stage(q):
        for n in range(4):
            c = 4 * q + n
            picked_f[q, n] = picked_f[q, n] + pick(0, (6, 7), pos_f[pl.ds(c, 1), :])
            row = pp[pl.ds(c, 1), 0, :].astype(f32)
            tgt_p[q, n] = jnp.broadcast_to(row, (128, CAPP)).T
        for m in range(2):
            picked_p[q, m] = pick(16, (0, 1), parent_place(2 * q + m))

    by_fours(last_stage)

    def transfer_stage(q):
        for n in range(4):
            carried_f[q, n] = carry_over(q, n, picked_f[q, n])

    by_fours(transfer_stage)

    plane = lax.broadcasted_iota(i32, (256, 128), 1).astype(f32)
    ones, zeros = jnp.ones((256, 128), f32), jnp.zeros((256, 128), f32)
    for n in range(3):
        total = None
        for c in range(CLASSES):
            spread = tgt_f[c // 4, c % 4]
            hot = jnp.concatenate(
                [
                    jnp.where(plane + (n * 256.0 + m) == spread, ones, zeros).astype(bf16)
                    for m in (0.0, 128.0)
                ],
                axis=1,
            )
            part = dot(carried_f[c // 4, c % 4], hot)
            total = part if total is None else total + part
        summed = total[0:COEF, :] + total[COEF : 2 * COEF, :]
        summed = jnp.concatenate([summed, jnp.zeros((104, 256), f32)], axis=0)
        turned_back = summed.T
        sums[0, n * 256 : n * 256 + 256, :] = turned_back[:, 0:128]
        sums[1, n * 256 : n * 256 + 256, :] = turned_back[:, 128:256]

    arrive(c_parent)
    doubled(20, 21)

    def parent_stage(q):
        for m in range(2):
            g = pick(16, (2,), parent_place(2 * q + m))
            picked_p[q, m] = picked_p[q, m] + g

    by_fours(parent_stage, unroll=2)

    def parent_transfer(q):
        for m in range(2):
            g = picked_p[q, m]
            carried_p[q, m] = jnp.concatenate(
                [carry_over(q, 2 * m, g[:, 0:128]), carry_over(q, 2 * m + 1, g[:, 128:256])],
                axis=1,
            )

    by_fours(parent_transfer, unroll=2)

    total = None
    for h in range(CLASSES // 2):
        hot = jnp.concatenate(
            [
                jnp.where(plane[0:CAPP] == tgt_p[c // 4, c % 4], 1.0, 0.0).astype(bf16)
                for c in (2 * h, 2 * h + 1)
            ],
            axis=0,
        )
        part = dot(carried_p[h // 2, h % 2], hot)
        total = part if total is None else total + part
    psum[0:COEF, :] = total[0:COEF, :] + total[COEF : 2 * COEF, :]
    loads[7].wait()
    expansion = coarse[...] + LEVEL_SCALE * psum[...].T[0:96, 0:COEF]
    lhi, llo = split(expansion)
    local[0] = lhi
    local[1] = llo

    for copies in (y_first, y_second, x_fine, x_parent, c_fine, c_parent):
        for copy, sends, _ in copies:

            @pl.when(sends)
            def _():
                copy.wait_send()


def finish(sums, local, dmaps, mask, out_hbm, rows, out, sem):
    pad = jnp.zeros((96, 256 - COEF), f32)
    lhi = local[0]
    lboth = jnp.concatenate([local[0], local[1]], axis=0)
    rows[...] = sums[...]
    pushed = []
    for k in range(8):
        both = dot(lboth, dmaps[k, 0])
        p = both[0:96, :] + (both[96:192, :] + dot(lhi, dmaps[k, 1]))
        pushed.append(jnp.concatenate([p, pad], axis=1))
    mask_t = mask[...]
    copies = []
    for px in range(3):
        for k in range(8):
            ci, cj, ck = k >> 2, (k >> 1) & 1, k & 1
            for py in range(4):
                at = pl.ds((2 * px + ci) * 128 + (2 * py + cj) * 16 + ck, 8, stride=2)
                n = (px * 4 + py) * 8
                rows[0, at, :] = rows[0, at, :] + pushed[k][n : n + 8, 0:128]
                rows[1, at, :] = rows[1, at, :] + pushed[k][n : n + 8, 128:256]
        for n in range(px * 16, px * 16 + 16):
            keep = mask_t[:, n : n + 1] > 0
            at = pl.ds(n * 16, 16)
            here = jnp.concatenate([rows[0, at, :], rows[1, at, :]], axis=1)[:, 0:COEF]
            out[at, :] = jnp.where(keep, here, jnp.zeros_like(here))
        part = pl.ds(px * 256, 256)
        copy = pltpu.make_async_copy(out.at[part], out_hbm.at[part], sem.at[px])
        copy.start()
        copies.append(copy)
    for copy in copies:
        copy.wait()


def per_device(shape, dens, occ, coarse, up, maps, down, fp, pp):
    vmem = pl.BlockSpec(memory_space=pltpu.VMEM)
    parts = pl.pallas_call(
        functools.partial(kernel, shape),
        out_shape=(
            jax.ShapeDtypeStruct((2, 768, 128), f32),
            jax.ShapeDtypeStruct((2, 96, COEF), bf16),
            jax.ShapeDtypeStruct((8, 2, COEF, COEF), bf16),
            jax.ShapeDtypeStruct((16, 128), f32),
        ),
        in_specs=[pl.BlockSpec(memory_space=pltpu.HBM)] * 8,
        out_specs=(vmem,) * 4,
        scratch_shapes=[
            pltpu.VMEM((768, COEF), f32),
            pltpu.VMEM((8, COEF, COEF), f32),
            pltpu.VMEM((CLASSES, COEF, COEF), f32),
            pltpu.VMEM((8, COEF, COEF), f32),
            pltpu.VMEM((48, 16), i32),
            pltpu.VMEM((96, COEF), f32),
            pltpu.VMEM((CLASSES, 2, CAPF), i32),
            pltpu.VMEM((CLASSES, 2, CAPP), i32),
            pltpu.VMEM((128, 128), f32),
            pltpu.VMEM((2, 768, 128), f32),
            pltpu.VMEM((TILES, COEF, 128), f32),
            pltpu.VMEM((TILES, 2 * COEF, 128), bf16),
            pltpu.VMEM((6, COEF, 128), f32),
            pltpu.VMEM((2, 512, 256), f32),
            pltpu.VMEM((4, 4, 160, 512), bf16),
            pltpu.VMEM((4, 4, CAPF, 128), f32),
            pltpu.VMEM((4, 4, CAPP, 128), f32),
            pltpu.VMEM((CLASSES, CAPF), i32),
            pltpu.VMEM((CLASSES, CAPP), i32),
            pltpu.VMEM((4, 4, 2 * COEF, CAPF), bf16),
            pltpu.VMEM((4, 2, 2 * COEF, 256), bf16),
            pltpu.VMEM((4, 4, 2 * COEF, CAPF), bf16),
            pltpu.VMEM((4, 2, 2 * COEF, 256), bf16),
            pltpu.VMEM((256, 128), f32),
            pltpu.SemaphoreType.DMA((8,)),
            pltpu.SemaphoreType.DMA((12,)),
            pltpu.SemaphoreType.DMA((12,)),
        ],
        compiler_params=pltpu.CompilerParams(
            collective_id=0, has_side_effects=True, vmem_limit_bytes=32 * 1024 * 1024
        ),
    )(
        *[pltpu.with_memory_space_constraint(v, pltpu.HBM) for v in (dens.reshape(768, COEF),
        occ.reshape(48, 16),
        coarse.reshape(96, COEF),
        up,
        maps,
        down,
        fp[0, 0],
        pp[0, 0])],
    )
    out = pl.pallas_call(
        finish,
        out_shape=jax.ShapeDtypeStruct((768, COEF), f32),
        in_specs=[vmem] * 4,
        out_specs=pl.BlockSpec(memory_space=pltpu.HBM),
        scratch_shapes=[
            pltpu.VMEM((2, 768, 128), f32),
            pltpu.VMEM((768, COEF), f32),
            pltpu.SemaphoreType.DMA((3,)),
        ],
        compiler_params=pltpu.CompilerParams(vmem_limit_bytes=8 * 1024 * 1024),
    )(*parts)
    return out.reshape(dens.shape)


def solution(mesh):
    shape = (mesh.shape["gx"], mesh.shape["gy"])
    return jax.shard_map(
        functools.partial(per_device, shape),
        mesh=mesh,
        in_specs=(
            P("gx", "gy", None, None),
            P("gx", "gy", None),
            P("gx", "gy", None, None),
            P(),
            P(),
            P(),
            P("gx", "gy", None, None, None),
            P("gx", "gy", None, None, None),
        ),
        out_specs=P("gx", "gy", None, None),
        check_vma=False,
    )
```
